32 devices in a mesh: blk: 16 (over z, y, x), auth: 2 (over core).
Axes of the slice: x: 2, y: 2, z: 4, core: 2. Of those that a mesh axis runs over, the one named last changes fastest.
Arguments:
- features: bfloat16 [2048, 1024], P('blk', 'auth'), may hold values from -6 to 6
- partners: int32 [16, 8], P('blk'), may hold values from 0 to 15, as said below
- tiles: bfloat16 [16, 8, 128, 128], P('blk'), may hold values from -0.125 to 0.125
- paper_w_in: bfloat16 [1024, 2048], P(None, 'auth'), may hold values from -0.1875 to 0.1875
- paper_w_out: bfloat16 [2048, 1024], P('auth'), may hold values from -0.125 to 0.125
- paper_gain: float32 [1024], replicated, may hold values from 0.5 to 1.5
- author_feats: bfloat16 [2048, 1024], P('blk', 'auth'), may hold values from -6 to 6
- assign: int32 [2048], P('blk'), may hold values from 0 to 127
- author_w_in: bfloat16 [1024, 2048], P(None, 'auth'), may hold values from -0.1875 to 0.1875
- author_w_out: bfloat16 [2048, 1024], P('auth'), may hold values from -0.125 to 0.125
- author_gain: float32 [1024], replicated, may hold values from 0.5 to 1.5
Outputs:
- paper_out: bfloat16 [2048, 1024], P('blk', 'auth')
- author_out: bfloat16 [2048, 1024], P('blk', 'auth')
The draws below stay inside these ranges and needn't reach their ends.
Inputs may be any that keep to these rules, and one draw needn't show every extreme that they name: `partners`: each row names 8 different blocks and never its own; block c names block b exactly when block b names block c.
All inputs are finite; a program needn't handle non-finite values.
Results may differ from the reference program's by a relative error of at most 0.013.
Values may be sent and summed in bfloat16 or wider, within the bound.
A program may use at most 128 MiB of HBM per device.

```python
import jax
import jax.numpy as jnp
from jax import lax

D = 1024
FF = 2048
R = 128
A_DEV = 128
BLOCKS = 16
PAPERS = 2048
PARTNERS = 8
AUTHORS = 2048


def draw_partners(key, part):
    count = BLOCKS
    modulus = count - 1
    round_key = jax.random.fold_in(key, 11)
    label_key = jax.random.fold_in(key, 12)
    order_key = jax.random.fold_in(key, 13)
    chosen = jax.random.permutation(round_key, modulus)[:PARTNERS].astype(jnp.int32)
    labels = jax.random.permutation(label_key, count).astype(jnp.int32)
    vertex = jnp.arange(count, dtype=jnp.int32)[:, None]
    rounds = chosen[None, :]
    mirror = jnp.mod(2 * rounds - vertex, modulus)
    other = jnp.where(vertex == modulus, rounds, jnp.where(vertex == rounds, modulus, mirror))
    labelled = labels[other]
    inverse = jnp.argsort(labels)
    table = labelled[inverse]
    keys = jax.random.split(order_key, count)
    shuffles = jax.vmap(lambda single: jax.random.permutation(single, PARTNERS))(keys)
    return jnp.take_along_axis(table, shuffles, axis=1).astype(jnp.int32)


def with_ends(array, rng, low, top_value):
    index_at = [jax.random.randint(jax.random.fold_in(rng, axis), (), 0, length) for axis, length in enumerate(array.shape)]
    main_axis = array.shape.index(max(array.shape))
    next_to = index_at[:main_axis] + [(index_at[main_axis] + 1) % array.shape[main_axis]] + index_at[main_axis + 1:]
    return array.at[tuple(index_at)].set(low).at[tuple(next_to)].set(top_value)


def levels(stream_key, dims, cuts, low, largest):
    def one(axis_at, shards_of):
        steps = jax.random.uniform(jax.random.fold_in(jax.random.fold_in(stream_key, 6), axis_at), (shards_of,), jnp.float32, low / len(cuts), largest / len(cuts))
        return jnp.repeat(jnp.exp(steps), dims[axis_at] // shards_of).reshape((-1,) + (1,) * (len(dims) - axis_at - 1))

    factor_of = one(*cuts[0])
    for cut in cuts[1:]:
        factor_of = factor_of * one(*cut)
    return factor_of


def noise(key, extent, spread, most, shards=(), held_as=jnp.bfloat16):
    drawn = spread * jax.random.normal(key, extent, jnp.float32)
    if shards:
        drawn = drawn * levels(key, extent, shards, -0.22, 0.18)
    return jnp.clip(drawn, -most, most).astype(held_as)


def setup_inputs(seed: int = 0) -> dict:
    seeds = jax.random.split(jax.random.key(seed), 12)
    features = noise(seeds[0], (PAPERS, D), 1.0, 6.0, ((0, 16), (1, 2)))
    partners = draw_partners(jax.random.fold_in(seeds[11], 71), 0)
    tiles = noise(seeds[2], (BLOCKS, PARTNERS, R, R), (2 * PARTNERS * R) ** -0.5, 0.125, ((0, 16),))
    paper_w_in = noise(seeds[3], (D, FF), D ** -0.5, 0.1875, ((1, 2),))
    paper_w_out = noise(seeds[4], (FF, D), FF ** -0.5, 0.125, ((0, 2),))
    paper_gain = jnp.clip(1.0 + 0.1 * jax.random.normal(seeds[5], (D,), jnp.float32), 0.5, 1.5)
    author_feats = noise(seeds[6], (AUTHORS, D), 1.0, 6.0, ((0, 16), (1, 2)))
    assign = with_ends(jax.random.randint(seeds[7], (PAPERS,), 0, A_DEV), jax.random.fold_in(seeds[7], 1), 0, A_DEV - 1).astype(jnp.int32)
    author_w_in = noise(seeds[8], (D, FF), D ** -0.5, 0.1875, ((1, 2),))
    author_w_out = noise(seeds[9], (FF, D), FF ** -0.5, 0.125, ((0, 2),))
    author_gain = jnp.clip(1.0 + 0.1 * jax.random.normal(seeds[10], (D,), jnp.float32), 0.5, 1.5)
    return {"features": features, "partners": partners, "tiles": tiles, "paper_w_in": paper_w_in, "paper_w_out": paper_w_out, "paper_gain": paper_gain, "author_feats": author_feats, "assign": assign, "author_w_in": author_w_in, "author_w_out": author_w_out, "author_gain": author_gain}


epsilon = 1e-06

def feed_forward(inputs, w_in, w_out, gain):
    values = inputs.astype(jnp.float32)
    square = lax.optimization_barrier(jnp.mean(values * values, axis=-1, keepdims=True))
    normed = (values * lax.rsqrt(square + epsilon) * gain).astype(jnp.bfloat16)
    hidden = jax.nn.silu(jnp.dot(normed, w_in, preferred_element_type=jnp.float32)).astype(jnp.bfloat16)
    return jnp.dot(hidden, w_out, preferred_element_type=jnp.float32)

def reference(features, partners, tiles, paper_w_in, paper_w_out, paper_gain, author_feats, assign, author_w_in, author_w_out, author_gain):
    blocks = features.reshape(BLOCKS, R, D)

    def block_sum(index):
        partner_ids = partners[index]
        linked = blocks[partner_ids].astype(jnp.float32)
        back_slot = jnp.argmax(partners[partner_ids] == index, axis=1).astype(jnp.int32)
        own_tiles = tiles[index].astype(jnp.float32)
        back_tiles = tiles[partner_ids, back_slot].astype(jnp.float32)
        forward = jnp.einsum('fij,fjd->fid', own_tiles, linked)
        reverse = jnp.einsum('fji,fjd->fid', back_tiles, linked)
        messages = (forward + reverse).astype(jnp.bfloat16)
        return lax.optimization_barrier(jnp.sum(messages.astype(jnp.float32), axis=0))
    gathered_sum = lax.map(block_sum, jnp.arange(BLOCKS, dtype=jnp.int32)).reshape(PAPERS, D)
    paper_pre = (features.astype(jnp.float32) + gathered_sum).astype(jnp.bfloat16)
    paper_mid = (paper_pre.astype(jnp.float32) + feed_forward(paper_pre, paper_w_in, paper_w_out, paper_gain)).astype(jnp.bfloat16)
    member = (assign.reshape(BLOCKS, 1, R) == jnp.arange(A_DEV, dtype=jnp.int32)[None, :, None]).astype(jnp.float32)
    author_sum = jnp.einsum('bar,brd->bad', member, paper_mid.reshape(BLOCKS, R, D).astype(jnp.float32))
    counts = lax.optimization_barrier(jnp.sum(member, axis=2))[:, :, None]
    average = (author_sum / jnp.maximum(counts, 1.0)).reshape(AUTHORS, D)
    author_pre = (author_feats.astype(jnp.float32) + average).astype(jnp.bfloat16)
    author_out = (author_pre.astype(jnp.float32) + feed_forward(author_pre, author_w_in, author_w_out, author_gain)).astype(jnp.bfloat16)
    returned = jnp.einsum('bar,bad->brd', member, author_out.reshape(BLOCKS, A_DEV, D).astype(jnp.float32)).reshape(PAPERS, D)
    paper_out = (paper_mid.astype(jnp.float32) + returned).astype(jnp.bfloat16)
    return (paper_out, author_out)
```

```python
import functools

import jax
import jax.numpy as jnp
from jax import lax
from jax.experimental import pallas as pl
from jax.experimental.pallas import tpu as pltpu
from jax.sharding import PartitionSpec as P

epsilon = 1e-06
MESH = pl.DeviceIdType.MESH


def plane_dims(count):
    if count % 4 == 0 and count <= 32:
        return (count // 4, 2, 2)
    return None


def kernel(
    count,
    partners_ref,
    tiles_ref,
    feat_ref,
    p_in_hbm,
    p_out_hbm,
    p_gain_ref,
    afeat_ref,
    assign_ref,
    a_in_hbm,
    a_out_hbm,
    a_gain_ref,
    result_ref,
    w_p_in,
    w_p_out,
    w_a_in,
    w_a_out,
    dense,
    back,
    linked,
    mixed,
    pre,
    partial_send,
    partial_recv,
    afeat_other,
    apart_send,
    apart_recv,
    mid,
    w_sem,
    relay_send,
    relay_recv,
    tile_send,
    tile_recv,
    core_send,
    core_recv,
    gossip,
    total_ref,
):
    rows, width = feat_ref.shape
    half = rows // 2
    me = lax.axis_index("blk")
    core = lax.axis_index("auth")
    other = 1 - core
    slots = partners_ref.shape[1]

    weights = [
        pltpu.make_async_copy(source, target, w_sem.at[slot])
        for slot, (source, target) in enumerate(
            ((p_in_hbm, w_p_in), (p_out_hbm, w_p_out), (a_in_hbm, w_a_in), (a_out_hbm, w_a_out))
        )
    ]

    dims = plane_dims(count)
    barrier = pltpu.get_barrier_semaphore()

    def signal(semaphore, block):
        pl.semaphore_signal(semaphore, inc=1, device_id={"blk": block}, device_id_type=MESH)

    if dims is None:

        def greet(step, carry):
            signal(barrier, lax.rem(me + step, count))
            return carry

        lax.fori_loop(1, count, greet, 0)
        near = count - 1
    else:
        depth = dims[0]
        plane = 4
        z = me // plane
        y = lax.rem(me // 2, 2)
        x = lax.rem(me, 2)
        near = 2 + (z > 0).astype(jnp.int32) + (z < depth - 1).astype(jnp.int32)

        def signal_near(semaphore):
            signal(semaphore, me + 1 - 2 * x)
            signal(semaphore, me + 2 - 4 * y)
            pl.when(z > 0)(lambda: signal(semaphore, me - plane))
            pl.when(z < depth - 1)(lambda: signal(semaphore, me + plane))

        signal_near(barrier)
    pl.semaphore_signal(barrier, inc=1, device_id={"auth": other}, device_id_type=MESH)

    def fill(block, carry):
        index = jnp.int32(0)
        found = jnp.int32(0)
        for slot in range(slots):
            same = (partners_ref[0, slot] == block).astype(jnp.int32)
            index = jnp.maximum(index, same * slot)
            found = jnp.maximum(found, same)
        tile = tiles_ref[0, index].astype(jnp.float32) * found.astype(jnp.float32)
        tile = tile.astype(jnp.bfloat16)
        dense[0, block] = tile[:half]
        dense[1, block] = tile[half:]
        return carry

    linked[pl.ds(pl.multiple_of(me * rows, rows), rows), :] = feat_ref[...]
    back[core, me] = jnp.zeros((half, rows), jnp.bfloat16)

    pl.semaphore_wait(barrier, near + 1)

    def to_core(source, target, slot):
        return pltpu.make_async_remote_copy(
            src_ref=source,
            dst_ref=target,
            send_sem=core_send.at[slot],
            recv_sem=core_recv.at[slot],
            device_id={"auth": other},
            device_id_type=MESH,
        )

    def tile_copy(step):
        block = lax.rem(me + step, count)
        return pltpu.make_async_remote_copy(
            src_ref=dense.at[core, block],
            dst_ref=back.at[core, me],
            send_sem=tile_send.at[step],
            recv_sem=tile_recv.at[step],
            device_id={"blk": block},
            device_id_type=MESH,
        )

    def start_tiles():
        if dims is not None:
            signal_near(gossip.at[0])
        lax.fori_loop(0, count, fill, 0)
        if dims is not None:
            for turn in range(depth):
                pl.semaphore_wait(gossip.at[turn], near)
                if turn < depth - 1:
                    signal_near(gossip.at[turn + 1])

        def one(step, carry):
            tile_copy(step).start()
            return carry

        lax.fori_loop(1, count, one, 0)

    afeat_copy = to_core(afeat_ref, afeat_other, 0)
    back_copy = to_core(back.at[core], back.at[core], 1)

    def finish_tiles():
        def one(step, carry):
            tile_copy(step).wait()
            return carry

        lax.fori_loop(1, count, one, 0)
        back_copy.start()

    def mix_tiles():
        back_copy.wait()

        def one(block, carry):
            own = jnp.concatenate([dense[0, block], dense[1, block]], axis=0)
            came = jnp.concatenate([back[0, block], back[1, block]], axis=0)
            whole = own.astype(jnp.float32) + came.astype(jnp.float32).T
            mixed[:, pl.ds(pl.multiple_of(block * rows, rows), rows)] = whole.astype(jnp.bfloat16)
            return carry

        lax.fori_loop(0, count, one, 0)

    if dims is None:

        def direct(step):
            return pltpu.make_async_remote_copy(
                src_ref=feat_ref,
                dst_ref=linked.at[pl.ds(pl.multiple_of(me * rows, rows), rows)],
                send_sem=relay_send.at[step],
                recv_sem=relay_recv.at[step],
                device_id={"blk": lax.rem(me + step, count)},
                device_id_type=MESH,
            )

        def start_one(step, carry):
            direct(step).start()
            return carry

        def wait_one(step, carry):
            direct(step).wait()
            return carry

        lax.fori_loop(1, count, start_one, 0)
        start_tiles()
        afeat_copy.start()
        for weight in weights:
            weight.start()
        finish_tiles()
        mix_tiles()
        lax.fori_loop(1, count, wait_one, 0)
    else:
        KINDS = {"up": 0, "down": 1, "x": 2, "y": 3, "far": 4}

        def move(kind, level, part):
            if kind == "up":
                origin, target, arrive = (y, x), me + plane, "col"
            elif kind == "down":
                origin, target, arrive = (y, x), me - plane, "col"
            elif kind == "x":
                origin, target, arrive = (y, x), me + 1 - 2 * x, "x"
            elif kind == "y":
                origin, target, arrive = (y, x), me + 2 - 4 * y, "y"
            elif part == 0:
                origin, target, arrive = (y, 1 - x), me + 2 - 4 * y, "far"
            else:
                origin, target, arrive = (1 - y, x), me + 1 - 2 * x, "far"
            block = level * plane + origin[0] * 2 + origin[1]
            place = pl.ds(pl.multiple_of(block * rows + part * half, half), half)
            spot = (level * 2 + part) * 5
            return pltpu.make_async_remote_copy(
                src_ref=linked.at[place],
                dst_ref=linked.at[place],
                send_sem=relay_send.at[spot + KINDS[kind]],
                recv_sem=relay_recv.at[(level * 2 + part) * 4 + ("col", "x", "y", "far").index(arrive)],
                device_id={"blk": target},
                device_id_type=MESH,
            )

        def arrived(arrive, level, part):
            origin = {"col": (y, x), "x": (y, 1 - x), "y": (1 - y, x), "far": (1 - y, 1 - x)}[arrive]
            block = level * plane + origin[0] * 2 + origin[1]
            place = pl.ds(pl.multiple_of(block * rows + part * half, half), half)
            pltpu.make_async_copy(
                linked.at[place],
                linked.at[place],
                relay_recv.at[(level * 2 + part) * 4 + ("col", "x", "y", "far").index(arrive)],
            ).wait()

        def levels(distance):
            if distance == 0:
                return ((z, None),)
            return ((z - distance, z >= distance), (z + distance, z < depth - distance))

        def when(condition, body):
            if condition is None:
                body()
            else:
                pl.when(condition)(body)

        def column(distance):
            for part in range(2):
                for side, (level, valid) in enumerate(levels(distance)):

                    def body(level=level, side=side, part=part):
                        arrived("col", level, part)
                        if side == 0:
                            pl.when(z < depth - 1)(lambda: move("up", level, part).start())
                        else:
                            pl.when(z > 0)(lambda: move("down", level, part).start())
                        move("x", level, part).start()
                        move("y", level, part).start()

                    when(valid, body)

        def beside(distance):
            for level, valid in levels(distance):

                def body(level=level):
                    arrived("x", level, 0)
                    move("far", level, 0).start()
                    arrived("y", level, 1)
                    move("far", level, 1).start()

                when(valid, body)

        for part in range(2):
            pl.when(z < depth - 1)(lambda part=part: move("up", z, part).start())
            pl.when(z > 0)(lambda part=part: move("down", z, part).start())
            first, second = ("x", "y") if part == 0 else ("y", "x")
            move(first, z, part).start()
            move(second, z, part).start()
        afeat_copy.start()
        for weight in weights:
            weight.start()
        start_tiles()
        total_ref[...] = feat_ref[...].astype(jnp.float32)

        def gather(distance):
            for level, valid in levels(distance):

                def rest(level=level):
                    for arrive, part in (("x", 1), ("y", 0), ("far", 0), ("far", 1)):
                        arrived(arrive, level, part)
                    span = plane * rows
                    start = pl.multiple_of(level * span, span)
                    total_ref[...] += jnp.dot(
                        mixed[:, pl.ds(start, span)],
                        linked[pl.ds(start, span), :],
                        preferred_element_type=jnp.float32,
                    )

                when(valid, rest)

        for distance in range(1, depth + 1):
            if distance < depth:
                column(distance)
            beside(distance - 1)
            if distance == max(depth - 2, 1):
                finish_tiles()
            if distance == max(depth - 1, 1):
                mix_tiles()
                for earlier in range(depth - 2):
                    gather(earlier)
        for distance in range(max(depth - 2, 0), depth):
            gather(distance)

    if dims is None:
        span = min(count * rows, 2048)

        def product(step, total):
            start = pl.multiple_of(step * span, span)
            return total + jnp.dot(
                mixed[:, pl.ds(start, span)],
                linked[pl.ds(start, span), :],
                preferred_element_type=jnp.float32,
            )

        total = feat_ref[...].astype(jnp.float32)
        total = lax.fori_loop(0, count * rows // span, product, total)
    else:
        total = total_ref[...]
    pre[core] = total.astype(jnp.bfloat16)
    pre_copy = to_core(pre.at[core], pre.at[core], 2)
    pre_copy.start()

    member = assign_ref[...] == lax.broadcasted_iota(jnp.int32, (afeat_ref.shape[0], rows), 0)
    member_wide = member.astype(jnp.float32)
    counts = jnp.maximum(jnp.sum(member_wide, axis=1, keepdims=True), 1.0)
    member_matrix = member_wide.astype(jnp.bfloat16)

    def hidden_of(left, right, w_in, gain):
        left = left.astype(jnp.float32)
        right = right.astype(jnp.float32)
        square = jnp.sum(left * left, axis=-1, keepdims=True)
        square = square + jnp.sum(right * right, axis=-1, keepdims=True)
        scale = lax.rsqrt(square / (2 * width) + epsilon)
        left = (left * scale * gain[:, :width]).astype(jnp.bfloat16)
        right = (right * scale * gain[:, width:]).astype(jnp.bfloat16)
        normed = jnp.concatenate([left, right], axis=1)
        units = jnp.dot(normed, w_in[...], preferred_element_type=jnp.float32)
        return (units / (1.0 + jnp.exp(-units))).astype(jnp.bfloat16)

    weights[0].wait()

    def scaled_units(side):
        values = pre[side].astype(jnp.float32)
        columns = pl.ds(pl.multiple_of(side * width, width), width)
        weighed = (values * p_gain_ref[:, columns]).astype(jnp.bfloat16)
        units = jnp.dot(weighed, w_p_in[columns, :], preferred_element_type=jnp.float32)
        return units, jnp.sum(values * values, axis=-1, keepdims=True)

    own_units, own_square = scaled_units(core)
    pre_copy.wait()
    far_units, far_square = scaled_units(other)
    scale = lax.rsqrt((own_square + far_square) / (2 * width) + epsilon)
    units = (own_units + far_units) * scale
    hidden = (units / (1.0 + jnp.exp(-units))).astype(jnp.bfloat16)
    weights[1].wait()
    terms = []
    partial_copies = []
    for side in range(2):
        term = jnp.dot(
            hidden,
            w_p_out[:, side * width : (side + 1) * width],
            preferred_element_type=jnp.float32,
        )
        terms.append(term)
        partial_send[side] = term.astype(jnp.bfloat16)
        copy = to_core(partial_send.at[side], partial_recv.at[side], 3 + side)
        copy.start()
        partial_copies.append(copy)
    afeat_copy.wait()
    author_pre = []
    for side in range(2):
        partial_copies[side].wait()
        sum_of = pre[side].astype(jnp.float32) + (
            terms[side] + partial_recv[side].astype(jnp.float32)
        )
        mid_side = sum_of.astype(jnp.bfloat16)
        mid[side] = mid_side
        author_sum = jnp.dot(member_matrix, mid_side, preferred_element_type=jnp.float32)
        mine = (core == side).astype(jnp.float32)
        base = afeat_ref[...].astype(jnp.float32) * mine
        base = base + afeat_other[...].astype(jnp.float32) * (1.0 - mine)
        author_pre.append((base + author_sum / counts).astype(jnp.bfloat16))
    weights[2].wait()
    hidden = hidden_of(author_pre[0], author_pre[1], w_a_in, a_gain_ref[...])
    weights[3].wait()
    theirs = pl.ds(pl.multiple_of(other * width, width), width)
    ours = pl.ds(pl.multiple_of(core * width, width), width)
    apart_send[...] = jnp.dot(
        hidden, w_a_out[:, theirs], preferred_element_type=jnp.float32
    ).astype(jnp.bfloat16)
    apart_copy = to_core(apart_send, apart_recv, 5)
    apart_copy.start()
    term = jnp.dot(hidden, w_a_out[:, ours], preferred_element_type=jnp.float32)
    mine = (core == 0).astype(jnp.float32)
    own_pre = author_pre[0].astype(jnp.float32) * mine
    own_pre = own_pre + author_pre[1].astype(jnp.float32) * (1.0 - mine)
    apart_copy.wait()
    author_out = (own_pre + (term + apart_recv[...].astype(jnp.float32))).astype(jnp.bfloat16)
    result_ref[1] = author_out
    returned = lax.dot_general(
        member_matrix,
        author_out,
        (((0,), (0,)), ((), ())),
        preferred_element_type=jnp.float32,
    )
    result_ref[0] = (mid[core].astype(jnp.float32) + returned).astype(jnp.bfloat16)

    if dims is not None:
        for distance in range(depth):
            for side, (level, valid) in enumerate(levels(distance)):

                def sent(level=level, side=side, distance=distance):
                    for part in range(2):
                        if distance == 0 or side == 0:
                            pl.when(z < depth - 1)(lambda part=part: move("up", level, part).wait_send())
                        if distance == 0 or side == 1:
                            pl.when(z > 0)(lambda part=part: move("down", level, part).wait_send())
                        for kind in ("x", "y", "far"):
                            move(kind, level, part).wait_send()

                when(valid, sent)


def local(
    features,
    partners,
    tiles,
    paper_w_in,
    paper_w_out,
    paper_gain,
    author_feats,
    assign,
    author_w_in,
    author_w_out,
    author_gain,
):
    count = lax.axis_size("blk")
    rows, width = features.shape
    half = rows // 2
    bf16 = jnp.bfloat16
    vmem = pl.BlockSpec(memory_space=pltpu.VMEM)
    hbm = pl.BlockSpec(memory_space=pl.ANY)
    smem = pl.BlockSpec(memory_space=pltpu.SMEM)
    dims = plane_dims(count)
    sends = count if dims is None else dims[0] * 10
    receives = count if dims is None else dims[0] * 8
    rounds = 1 if dims is None else dims[0]
    (result,) = pl.pallas_call(
        functools.partial(kernel, count),
        out_shape=(pltpu.VMEM((2,) + features.shape, bf16),),
        in_specs=[smem, vmem, vmem, hbm, hbm, vmem, vmem, vmem, hbm, hbm, vmem],
        out_specs=(vmem,),
        scratch_shapes=[
            pltpu.VMEM(paper_w_in.shape, bf16),
            pltpu.VMEM(paper_w_out.shape, bf16),
            pltpu.VMEM(author_w_in.shape, bf16),
            pltpu.VMEM(author_w_out.shape, bf16),
            pltpu.VMEM((2, count, half, rows), bf16),
            pltpu.VMEM((2, count, half, rows), bf16),
            pltpu.VMEM((count * rows, width), bf16),
            pltpu.VMEM((rows, count * rows), bf16),
            pltpu.VMEM((2, rows, width), bf16),
            pltpu.VMEM((2, rows, width), bf16),
            pltpu.VMEM((2, rows, width), bf16),
            pltpu.VMEM(author_feats.shape, bf16),
            pltpu.VMEM(author_feats.shape, bf16),
            pltpu.VMEM(author_feats.shape, bf16),
            pltpu.VMEM((2, rows, width), bf16),
            pltpu.SemaphoreType.DMA((4,)),
            pltpu.SemaphoreType.DMA((sends,)),
            pltpu.SemaphoreType.DMA((receives,)),
            pltpu.SemaphoreType.DMA((count,)),
            pltpu.SemaphoreType.DMA((count,)),
            pltpu.SemaphoreType.DMA((6,)),
            pltpu.SemaphoreType.DMA((6,)),
            pltpu.SemaphoreType.REGULAR((rounds,)),
            pltpu.VMEM((rows, width), jnp.float32),
        ],
        compiler_params=pltpu.CompilerParams(
            collective_id=0, has_side_effects=True, vmem_limit_bytes=56 * 1024 * 1024
        ),
    )(
        partners,
        tiles,
        features,
        paper_w_in,
        paper_w_out,
        paper_gain[None, :],
        author_feats,
        assign[None, :],
        author_w_in,
        author_w_out,
        author_gain[None, :],
    )
    return result[0], result[1]


def solution(mesh):
    placed = (
        P("blk", "auth"),
        P("blk", None),
        P("blk", None, None, None),
        P(None, "auth"),
        P("auth", None),
        P(),
        P("blk", "auth"),
        P("blk"),
        P(None, "auth"),
        P("auth", None),
        P(),
    )
    return jax.shard_map(
        local,
        mesh=mesh,
        in_specs=placed,
        out_specs=(P("blk", "auth"), P("blk", "auth")),
        check_vma=False,
    )
```

```python
import functools

import jax
import jax.numpy as jnp
from jax import lax
from jax.experimental import pallas as pl
from jax.experimental.pallas import tpu as pltpu
from jax.sharding import PartitionSpec as P

epsilon = 1e-06
MESH = pl.DeviceIdType.MESH
LANES = 128
PLANE = 4
RING = 4


def to_other_core(source, target, send_sem, recv_sem, slot, other):
    return pltpu.make_async_remote_copy(
        src_ref=source,
        dst_ref=target,
        send_sem=send_sem.at[slot],
        recv_sem=recv_sem.at[slot],
        device_id={"auth": other},
        device_id_type=MESH,
    )


def membership(assign_ref, authors, rows):
    member = assign_ref[...] == lax.broadcasted_iota(jnp.int32, (authors, rows), 0)
    member_wide = member.astype(jnp.float32)
    counts = jnp.maximum(jnp.sum(member_wide, axis=1, keepdims=True), 1.0)
    return member_wide.astype(jnp.bfloat16), counts


def silu(units):
    return (units / (1.0 + jnp.exp(-units))).astype(jnp.bfloat16)


def scaled_units(pre, side, width, p_gain_ref, w_p_in):
    values = pre[side].astype(jnp.float32)
    columns = pl.ds(pl.multiple_of(side * width, width), width)
    weighed = (values * p_gain_ref[:, columns]).astype(jnp.bfloat16)
    units = jnp.dot(weighed, w_p_in[columns, :], preferred_element_type=jnp.float32)
    return units, jnp.sum(values * values, axis=-1, keepdims=True)


def after_hidden(
    core,
    hidden,
    member_matrix,
    counts,
    weights,
    to_core,
    slots,
    afeat,
    afeat_other,
    pre,
    w_p_out,
    w_a_in,
    w_a_out,
    a_gain_ref,
    partial_send,
    partial_recv,
    apart_send,
    apart_recv,
    mid,
    result_ref,
):
    other = 1 - core
    width = afeat.shape[1]
    weights[1].wait()
    terms = []
    partial_copies = []
    for side in range(2):
        term = jnp.dot(
            hidden,
            w_p_out[:, side * width : (side + 1) * width],
            preferred_element_type=jnp.float32,
        )
        terms.append(term)
        partial_send[side] = term.astype(jnp.bfloat16)
        copy = to_core(partial_send.at[side], partial_recv.at[side], slots[side])
        copy.start()
        partial_copies.append(copy)
    author_pre = []
    for side in range(2):
        partial_copies[side].wait()
        sum_of = pre[side].astype(jnp.float32) + (
            terms[side] + partial_recv[side].astype(jnp.float32)
        )
        mid_side = sum_of.astype(jnp.bfloat16)
        mid[side] = mid_side
        author_sum = jnp.dot(member_matrix, mid_side, preferred_element_type=jnp.float32)
        mine = (core == side).astype(jnp.float32)
        base = afeat[...].astype(jnp.float32) * mine
        base = base + afeat_other[...].astype(jnp.float32) * (1.0 - mine)
        author_pre.append((base + author_sum / counts).astype(jnp.bfloat16))
    weights[2].wait()
    left = author_pre[0].astype(jnp.float32)
    right = author_pre[1].astype(jnp.float32)
    square = jnp.sum(left * left, axis=-1, keepdims=True)
    square = square + jnp.sum(right * right, axis=-1, keepdims=True)
    scale = lax.rsqrt(square / (2 * width) + epsilon)
    gain = a_gain_ref[...]
    left = (left * scale * gain[:, :width]).astype(jnp.bfloat16)
    right = (right * scale * gain[:, width:]).astype(jnp.bfloat16)
    normed = jnp.concatenate([left, right], axis=1)
    hidden = silu(jnp.dot(normed, w_a_in[...], preferred_element_type=jnp.float32))
    weights[3].wait()
    theirs = pl.ds(pl.multiple_of(other * width, width), width)
    ours = pl.ds(pl.multiple_of(core * width, width), width)
    apart_send[...] = jnp.dot(
        hidden, w_a_out[:, theirs], preferred_element_type=jnp.float32
    ).astype(jnp.bfloat16)
    apart_copy = to_core(apart_send, apart_recv, slots[2])
    apart_copy.start()
    term = jnp.dot(hidden, w_a_out[:, ours], preferred_element_type=jnp.float32)
    mine = (core == 0).astype(jnp.float32)
    own_pre = author_pre[0].astype(jnp.float32) * mine
    own_pre = own_pre + author_pre[1].astype(jnp.float32) * (1.0 - mine)
    apart_copy.wait()
    author_out = (own_pre + (term + apart_recv[...].astype(jnp.float32))).astype(jnp.bfloat16)
    result_ref[1] = author_out
    returned = lax.dot_general(
        member_matrix,
        author_out,
        (((0,), (0,)), ((), ())),
        preferred_element_type=jnp.float32,
    )
    result_ref[0] = (mid[core].astype(jnp.float32) + returned).astype(jnp.bfloat16)


def grid_kernel(
    count,
    partners_ref,
    tiles_hbm,
    feat_hbm,
    p_in_hbm,
    p_out_hbm,
    p_gain_ref,
    afeat_hbm,
    assign_ref,
    a_in_hbm,
    a_out_hbm,
    a_gain_ref,
    result_ref,
    w_p_in,
    w_p_out,
    w_a_in,
    w_a_out,
    tiles,
    plane_tiles,
    ring_tiles,
    ahead,
    back,
    mixed,
    linked,
    product,
    part_send,
    part_recv,
    pre,
    partial_send,
    partial_recv,
    afeat,
    afeat_other,
    apart_send,
    apart_recv,
    mid,
    w_sem,
    load_sem,
    ring_send,
    ring_recv,
    tile_send,
    tile_recv,
    part_send_sem,
    part_recv_sem,
    core_send,
    core_recv,
):
    rows, width = afeat.shape
    half = rows // 2
    chunks = linked.shape[0]
    wide = width // chunks
    me = lax.axis_index("blk")
    core = lax.axis_index("auth")
    other = 1 - core
    slots = partners_ref.shape[1]
    z = me // PLANE
    y = lax.rem(me // 2, 2)
    x = lax.rem(me, 2)
    place = lax.rem(me, PLANE)

    def across(step):
        far_x = 1 - x if step % 2 else x
        far_y = 1 - y if step // 2 else y
        return far_y * 2 + far_x

    def level(step):
        return lax.rem(z + step, RING)

    def rows_of(index, size=rows):
        return pl.ds(pl.multiple_of(index * size, size), size)

    mine = rows_of(core, half)
    steps = range(1, PLANE)

    loads = [
        pltpu.make_async_copy(
            feat_hbm.at[:, n * wide : (n + 1) * wide],
            linked.at[n, rows_of(z)],
            load_sem.at[n],
        )
        for n in range(chunks)
    ]
    tile_load = pltpu.make_async_copy(tiles_hbm.at[0], tiles, load_sem.at[chunks])
    afeat_load = pltpu.make_async_copy(afeat_hbm, afeat, load_sem.at[chunks + 1])
    weights = [
        pltpu.make_async_copy(source, target, w_sem.at[slot])
        for slot, (source, target) in enumerate(
            ((p_in_hbm, w_p_in), (p_out_hbm, w_p_out), (a_in_hbm, w_a_in), (a_out_hbm, w_a_out))
        )
    ]

    barrier = pltpu.get_barrier_semaphore()
    for step in steps:
        for block in (z * PLANE + across(step), level(step) * PLANE + place):
            pl.semaphore_signal(barrier, inc=1, device_id={"blk": block}, device_id_type=MESH)
    pl.semaphore_signal(barrier, inc=1, device_id={"auth": other}, device_id_type=MESH)
    for load in loads:
        load.start()
    tile_load.start()
    afeat_load.start()

    def remote(source, target, send_sem, recv_sem, block):
        return pltpu.make_async_remote_copy(
            src_ref=source,
            dst_ref=target,
            send_sem=send_sem,
            recv_sem=recv_sem,
            device_id={"blk": block},
            device_id_type=MESH,
        )

    def arrived(target, semaphore):
        pltpu.make_async_copy(target, target, semaphore).wait()

    def to_core(source, target, slot):
        return to_other_core(source, target, core_send, core_recv, slot, other)

    even = 1 - lax.rem(z, 2)
    relay_from = lax.rem(z + 1 + 2 * even, RING)
    relay_to = lax.rem(z + 1 + 2 * (1 - even), RING)

    def ring_copy(kind, n):
        origin, target = (
            (z, level(1)),
            (z, level(RING - 1)),
            (relay_from, relay_to),
        )[kind]
        spot = linked.at[n, rows_of(origin)]
        return remote(
            spot,
            spot,
            ring_send.at[n * 3 + kind],
            ring_recv.at[n * RING + origin],
            target * PLANE + place,
        )

    def ring_arrived(n, origin):
        arrived(linked.at[n, rows_of(origin)], ring_recv.at[n * RING + origin])

    def plane_copy(step):
        return remote(
            plane_tiles.at[across(step), mine],
            ahead.at[place, mine],
            tile_send.at[step - 1],
            tile_recv.at[step - 1],
            z * PLANE + across(step),
        )

    def column_copy(step):
        return remote(
            ring_tiles.at[level(step), mine],
            back.at[z, mine],
            tile_send.at[PLANE + step - 1],
            tile_recv.at[PLANE + step - 1],
            level(step) * PLANE + place,
        )

    def part_copy(n, step):
        return remote(
            part_send.at[n, across(step)],
            part_recv.at[n, step - 1],
            part_send_sem.at[n * 3 + step - 1],
            part_recv_sem.at[n * 3 + step - 1],
            z * PLANE + across(step),
        )

    def start_own(n):
        ring_copy(0, n).start()
        ring_copy(1, n).start()

    def relay(n):
        ring_arrived(n, relay_from)
        ring_copy(2, n).start()

    for load in loads:
        load.wait()
    pl.semaphore_wait(barrier, 2 * (PLANE - 1) + 1)
    start_own(0)
    tile_load.wait()
    for block in range(count):
        index = jnp.int32(0)
        found = jnp.int32(0)
        for slot in range(slots):
            same = (partners_ref[0, slot] == block).astype(jnp.int32)
            index = jnp.maximum(index, same * slot)
            found = jnp.maximum(found, same)
        tile = tiles[index].astype(jnp.float32) * found.astype(jnp.float32)
        tile = tile.astype(jnp.bfloat16)
        upper, inner = block // PLANE, block % PLANE
        ring_tiles[upper, :, inner * rows : (inner + 1) * rows] = tile
        plane_tiles[inner, :, upper * rows : (upper + 1) * rows] = tile
    for step in (2, 1, 3):
        column_copy(step).start()
    for step in (3, 1, 2):
        plane_copy(step).start()
    start_own(1)
    for weight in weights:
        weight.start()
    afeat_load.wait()
    afeat_copy = to_core(afeat, afeat_other, 0)
    afeat_copy.start()

    relay(0)
    start_own(2)

    ahead[place] = plane_tiles[place]
    plane_exchange = []
    for step in steps:
        spot = ahead.at[across(step), mine]
        arrived(spot, tile_recv.at[step - 1])
        copy = to_core(spot, spot, step)
        copy.start()
        plane_exchange.append(copy)
    column_exchange = []
    for step in steps:
        spot = back.at[level(RING - step), mine]
        arrived(spot, tile_recv.at[PLANE + step - 1])
        copy = to_core(spot, spot, PLANE - 1 + step)
        copy.start()
        column_exchange.append(copy)
    relay(1)
    start_own(3)

    def mix(origin, came):
        columns = rows_of(origin)
        for inner in range(PLANE):
            own = ahead[inner, :, columns].astype(jnp.float32)
            there = came[origin, :, inner * rows : (inner + 1) * rows].astype(jnp.float32)
            mixed[inner * rows : (inner + 1) * rows, columns] = (own + there.T).astype(jnp.bfloat16)

    for copy in plane_exchange:
        copy.wait()
    mix(z, ring_tiles)
    for step in steps:
        column_exchange[step - 1].wait()
        mix(level(RING - step), back)

    def products(n):
        ring_arrived(n, relay_to)
        ring_arrived(n, level(2))
        total = jnp.dot(mixed[...], linked[n], preferred_element_type=jnp.float32)
        product[n] = total
        for inner in range(PLANE):
            part_send[n, inner] = total[inner * rows : (inner + 1) * rows].astype(jnp.bfloat16)
        for step in (3, 1, 2):
            part_copy(n, step).start()

    def collect(n):
        total = linked[n, rows_of(z)].astype(jnp.float32) + product[n, rows_of(place)]
        for step in steps:
            arrived(part_recv.at[n, step - 1], part_recv_sem.at[n * 3 + step - 1])
            total = total + part_recv[n, step - 1].astype(jnp.float32)
        spot = pre.at[core, :, n * wide : (n + 1) * wide]
        spot[...] = total.astype(jnp.bfloat16)
        copy = to_core(spot, spot, 2 * PLANE - 1 + n)
        copy.start()
        return copy

    def feed(side, start, stop):
        values = pre[side, :, start * wide : stop * wide].astype(jnp.float32)
        first = pl.multiple_of(side * width + start * wide, wide)
        columns = pl.ds(first, (stop - start) * wide)
        weighed = (values * p_gain_ref[:, columns]).astype(jnp.bfloat16)
        units = jnp.dot(weighed, w_p_in[columns, :], preferred_element_type=jnp.float32)
        return units, jnp.sum(values * values, axis=-1, keepdims=True)

    def add(units, square, more):
        return units + more[0], square + more[1]

    relay(2)
    products(0)
    products(1)
    relay(3)
    products(2)
    pre_copies = [collect(0), collect(1)]
    products(3)
    member_matrix, counts = membership(assign_ref, afeat.shape[0], rows)
    weights[0].wait()
    units, square = feed(core, 0, 2)
    for copy in pre_copies:
        copy.wait()
    units, square = add(units, square, feed(other, 0, 2))
    for n in range(2, chunks):
        copy = collect(n)
        units, square = add(units, square, feed(core, n, n + 1))
        copy.wait()
        units, square = add(units, square, feed(other, n, n + 1))
    hidden = silu(units * lax.rsqrt(square / (2 * width) + epsilon))
    afeat_copy.wait()
    last = 2 * PLANE - 1 + chunks
    after_hidden(
        core,
        hidden,
        member_matrix,
        counts,
        weights,
        to_core,
        (last, last + 1, last + 2),
        afeat,
        afeat_other,
        pre,
        w_p_out,
        w_a_in,
        w_a_out,
        a_gain_ref,
        partial_send,
        partial_recv,
        apart_send,
        apart_recv,
        mid,
        result_ref,
    )

    for n in range(chunks):
        for kind in range(3):
            ring_copy(kind, n).wait_send()
        for step in steps:
            part_copy(n, step).wait_send()
    for step in steps:
        plane_copy(step).wait_send()
        column_copy(step).wait_send()


def direct_kernel(
    count,
    partners_ref,
    tiles_ref,
    feat_ref,
    p_in_hbm,
    p_out_hbm,
    p_gain_ref,
    afeat_ref,
    assign_ref,
    a_in_hbm,
    a_out_hbm,
    a_gain_ref,
    result_ref,
    w_p_in,
    w_p_out,
    w_a_in,
    w_a_out,
    dense,
    back,
    linked,
    mixed,
    pre,
    partial_send,
    partial_recv,
    afeat_other,
    apart_send,
    apart_recv,
    mid,
    w_sem,
    relay_send,
    relay_recv,
    tile_send,
    tile_recv,
    core_send,
    core_recv,
):
    rows, width = feat_ref.shape
    half = rows // 2
    me = lax.axis_index("blk")
    core = lax.axis_index("auth")
    other = 1 - core
    slots = partners_ref.shape[1]

    weights = [
        pltpu.make_async_copy(source, target, w_sem.at[slot])
        for slot, (source, target) in enumerate(
            ((p_in_hbm, w_p_in), (p_out_hbm, w_p_out), (a_in_hbm, w_a_in), (a_out_hbm, w_a_out))
        )
    ]

    barrier = pltpu.get_barrier_semaphore()

    def greet(step, carry):
        block = lax.rem(me + step, count)
        pl.semaphore_signal(barrier, inc=1, device_id={"blk": block}, device_id_type=MESH)
        return carry

    lax.fori_loop(1, count, greet, 0)
    pl.semaphore_signal(barrier, inc=1, device_id={"auth": other}, device_id_type=MESH)

    def fill(block, carry):
        index = jnp.int32(0)
        found = jnp.int32(0)
        for slot in range(slots):
            same = (partners_ref[0, slot] == block).astype(jnp.int32)
            index = jnp.maximum(index, same * slot)
            found = jnp.maximum(found, same)
        tile = tiles_ref[0, index].astype(jnp.float32) * found.astype(jnp.float32)
        tile = tile.astype(jnp.bfloat16)
        dense[0, block] = tile[:half]
        dense[1, block] = tile[half:]
        return carry

    linked[pl.ds(pl.multiple_of(me * rows, rows), rows), :] = feat_ref[...]
    back[core, me] = jnp.zeros((half, rows), jnp.bfloat16)

    pl.semaphore_wait(barrier, count)

    def to_core(source, target, slot):
        return to_other_core(source, target, core_send, core_recv, slot, other)

    def tile_copy(step):
        block = lax.rem(me + step, count)
        return pltpu.make_async_remote_copy(
            src_ref=dense.at[core, block],
            dst_ref=back.at[core, me],
            send_sem=tile_send.at[step],
            recv_sem=tile_recv.at[step],
            device_id={"blk": block},
            device_id_type=MESH,
        )

    afeat_copy = to_core(afeat_ref, afeat_other, 0)
    back_copy = to_core(back.at[core], back.at[core], 1)

    def direct(step):
        return pltpu.make_async_remote_copy(
            src_ref=feat_ref,
            dst_ref=linked.at[pl.ds(pl.multiple_of(me * rows, rows), rows)],
            send_sem=relay_send.at[step],
            recv_sem=relay_recv.at[step],
            device_id={"blk": lax.rem(me + step, count)},
            device_id_type=MESH,
        )

    def run(body):
        def one(step, carry):
            body(step)
            return carry

        lax.fori_loop(1, count, one, 0)

    run(lambda step: direct(step).start())
    lax.fori_loop(0, count, fill, 0)
    run(lambda step: tile_copy(step).start())
    afeat_copy.start()
    for weight in weights:
        weight.start()
    run(lambda step: tile_copy(step).wait())
    back_copy.start()
    back_copy.wait()

    def mix(block, carry):
        own = jnp.concatenate([dense[0, block], dense[1, block]], axis=0)
        came = jnp.concatenate([back[0, block], back[1, block]], axis=0)
        whole = own.astype(jnp.float32) + came.astype(jnp.float32).T
        mixed[:, pl.ds(pl.multiple_of(block * rows, rows), rows)] = whole.astype(jnp.bfloat16)
        return carry

    lax.fori_loop(0, count, mix, 0)
    run(lambda step: direct(step).wait())

    span = min(count * rows, 2048)

    def product(step, total):
        start = pl.multiple_of(step * span, span)
        return total + jnp.dot(
            mixed[:, pl.ds(start, span)],
            linked[pl.ds(start, span), :],
            preferred_element_type=jnp.float32,
        )

    total = feat_ref[...].astype(jnp.float32)
    total = lax.fori_loop(0, count * rows // span, product, total)
    pre[core] = total.astype(jnp.bfloat16)
    pre_copy = to_core(pre.at[core], pre.at[core], 2)
    pre_copy.start()

    member_matrix, counts = membership(assign_ref, afeat_ref.shape[0], rows)
    weights[0].wait()
    own_units, own_square = scaled_units(pre, core, width, p_gain_ref, w_p_in)
    pre_copy.wait()
    far_units, far_square = scaled_units(pre, other, width, p_gain_ref, w_p_in)
    scale = lax.rsqrt((own_square + far_square) / (2 * width) + epsilon)
    hidden = silu((own_units + far_units) * scale)
    afeat_copy.wait()
    after_hidden(
        core,
        hidden,
        member_matrix,
        counts,
        weights,
        to_core,
        (3, 4, 5),
        afeat_ref,
        afeat_other,
        pre,
        w_p_out,
        w_a_in,
        w_a_out,
        a_gain_ref,
        partial_send,
        partial_recv,
        apart_send,
        apart_recv,
        mid,
        result_ref,
    )


def local(
    features,
    partners,
    tiles,
    paper_w_in,
    paper_w_out,
    paper_gain,
    author_feats,
    assign,
    author_w_in,
    author_w_out,
    author_gain,
):
    count = lax.axis_size("blk")
    rows, width = features.shape
    bf16 = jnp.bfloat16
    f32 = jnp.float32
    vmem = pl.BlockSpec(memory_space=pltpu.VMEM)
    hbm = pl.BlockSpec(memory_space=pl.ANY)
    smem = pl.BlockSpec(memory_space=pltpu.SMEM)
    dma = pltpu.SemaphoreType.DMA
    pair = pltpu.VMEM((2, rows, width), bf16)
    single = pltpu.VMEM(author_feats.shape, bf16)
    held = [
        pltpu.VMEM(paper_w_in.shape, bf16),
        pltpu.VMEM(paper_w_out.shape, bf16),
        pltpu.VMEM(author_w_in.shape, bf16),
        pltpu.VMEM(author_w_out.shape, bf16),
    ]
    if count == PLANE * RING and width % LANES == 0:
        chunks = width // LANES
        body = grid_kernel
        near = hbm
        scratch = held + [
            pltpu.VMEM(tiles.shape[1:], bf16),
            pltpu.VMEM((PLANE, rows, RING * rows), bf16),
            pltpu.VMEM((RING, rows, PLANE * rows), bf16),
            pltpu.VMEM((PLANE, rows, RING * rows), bf16),
            pltpu.VMEM((RING, rows, PLANE * rows), bf16),
            pltpu.VMEM((PLANE * rows, RING * rows), bf16),
            pltpu.VMEM((chunks, RING * rows, LANES), bf16),
            pltpu.VMEM((chunks, PLANE * rows, LANES), f32),
            pltpu.VMEM((chunks, PLANE, rows, LANES), bf16),
            pltpu.VMEM((chunks, PLANE - 1, rows, LANES), bf16),
            pair,
            pair,
            pair,
            single,
            single,
            single,
            single,
            pair,
            dma((4,)),
            dma((chunks + 2,)),
            dma((chunks * 3,)),
            dma((chunks * RING,)),
            dma((PLANE + RING,)),
            dma((PLANE + RING,)),
            dma((chunks * (PLANE - 1),)),
            dma((chunks * (PLANE - 1),)),
            dma((2 * PLANE + 2 + chunks,)),
            dma((2 * PLANE + 2 + chunks,)),
        ]
    else:
        body = direct_kernel
        near = vmem
        tile_half = pltpu.VMEM((2, count, rows // 2, rows), bf16)
        scratch = held + [
            tile_half,
            tile_half,
            pltpu.VMEM((count * rows, width), bf16),
            pltpu.VMEM((rows, count * rows), bf16),
            pair,
            pair,
            pair,
            single,
            single,
            single,
            pair,
            dma((4,)),
            dma((count,)),
            dma((count,)),
            dma((count,)),
            dma((count,)),
            dma((6,)),
            dma((6,)),
        ]
    (result,) = pl.pallas_call(
        functools.partial(body, count),
        out_shape=(pltpu.VMEM((2,) + features.shape, bf16),),
        in_specs=[smem, near, near, hbm, hbm, vmem, near, vmem, hbm, hbm, vmem],
        out_specs=(vmem,),
        scratch_shapes=scratch,
        compiler_params=pltpu.CompilerParams(
            collective_id=0, has_side_effects=True, vmem_limit_bytes=56 * 1024 * 1024
        ),
    )(
        partners,
        tiles,
        features,
        paper_w_in,
        paper_w_out,
        paper_gain[None, :],
        author_feats,
        assign[None, :],
        author_w_in,
        author_w_out,
        author_gain[None, :],
    )
    return result[0], result[1]


def solution(mesh):
    placed = (
        P("blk", "auth"),
        P("blk", None),
        P("blk", None, None, None),
        P(None, "auth"),
        P("auth", None),
        P(),
        P("blk", "auth"),
        P("blk"),
        P(None, "auth"),
        P("auth", None),
        P(),
    )
    return jax.shard_map(
        local,
        mesh=mesh,
        in_specs=placed,
        out_specs=(P("blk", "auth"), P("blk", "auth")),
        check_vma=False,
    )
```

```python
import functools

import jax
import jax.numpy as jnp
from jax import lax
from jax.experimental import pallas as pl
from jax.experimental.pallas import tpu as pltpu
from jax.sharding import PartitionSpec as P

epsilon = 1e-06
MESH = pl.DeviceIdType.MESH
LANES = 128
PLANE = 4
RING = 4


def to_other_core(source, target, send_sem, recv_sem, slot, other):
    return pltpu.make_async_remote_copy(
        src_ref=source,
        dst_ref=target,
        send_sem=send_sem.at[slot],
        recv_sem=recv_sem.at[slot],
        device_id={"auth": other},
        device_id_type=MESH,
    )


def membership(assign_ref, authors, rows):
    member = assign_ref[...] == lax.broadcasted_iota(jnp.int32, (authors, rows), 0)
    member_wide = member.astype(jnp.float32)
    counts = jnp.maximum(jnp.sum(member_wide, axis=1, keepdims=True), 1.0)
    return member_wide.astype(jnp.bfloat16), member_wide.T.astype(jnp.bfloat16), 1.0 / counts


def silu(units):
    part = 0.5 * units
    return (part + part * jnp.tanh(part)).astype(jnp.bfloat16)


def scaled_units(pre, side, width, p_gain_ref, w_p_in):
    values = pre[side].astype(jnp.float32)
    columns = pl.ds(pl.multiple_of(side * width, width), width)
    weighed = (values * p_gain_ref[:, columns]).astype(jnp.bfloat16)
    units = jnp.dot(weighed, w_p_in[columns, :], preferred_element_type=jnp.float32)
    return units, jnp.sum(values * values, axis=-1, keepdims=True)


def after_hidden(
    core,
    hidden,
    member_matrix,
    member_back,
    inverse,
    weights,
    to_core,
    slots,
    afeat,
    pre,
    w_p_out,
    w_a_in,
    w_a_out,
    a_gain_ref,
    partial_send,
    partial_recv,
    apart_send,
    apart_recv,
    mid,
    author_pre,
    result_ref,
):
    other = 1 - core
    width = afeat.shape[2]
    weights[1].wait()
    terms = []
    partial_copies = []
    for side in range(2):
        term = jnp.dot(
            hidden,
            w_p_out[:, side * width : (side + 1) * width],
            preferred_element_type=jnp.float32,
        )
        terms.append(term)
        partial_send[side] = term.astype(jnp.bfloat16)
        copy = to_core(partial_send.at[side], partial_recv.at[side], slots[side])
        copy.start()
        partial_copies.append(copy)
    terms = [terms[side] + pre[side].astype(jnp.float32) for side in range(2)]
    weights[2].wait()
    units = 0.0
    square = 0.0
    for side in range(2):
        columns = slice(side * width, (side + 1) * width)
        partial_copies[side].wait()
        mid_side = (terms[side] + partial_recv[side].astype(jnp.float32)).astype(jnp.bfloat16)
        mid[side] = mid_side
        author_sum = jnp.dot(member_matrix, mid_side, preferred_element_type=jnp.float32)
        whole = (afeat[side].astype(jnp.float32) + author_sum * inverse).astype(jnp.bfloat16)
        author_pre[side] = whole
        values = whole.astype(jnp.float32)
        weighed = (values * a_gain_ref[:, columns]).astype(jnp.bfloat16)
        units = units + jnp.dot(weighed, w_a_in[columns, :], preferred_element_type=jnp.float32)
        square = square + jnp.sum(values * values, axis=-1, keepdims=True)
    hidden = silu(units * lax.rsqrt(square / (2 * width) + epsilon))
    weights[3].wait()
    theirs = pl.ds(pl.multiple_of(other * width, width), width)
    ours = pl.ds(pl.multiple_of(core * width, width), width)
    apart_send[...] = jnp.dot(
        hidden, w_a_out[:, theirs], preferred_element_type=jnp.float32
    ).astype(jnp.bfloat16)
    apart_copy = to_core(apart_send, apart_recv, slots[2])
    apart_copy.start()
    term = jnp.dot(hidden, w_a_out[:, ours], preferred_element_type=jnp.float32)
    term = term + author_pre[core].astype(jnp.float32)
    apart_copy.wait()
    author_out = (term + apart_recv[...].astype(jnp.float32)).astype(jnp.bfloat16)
    result_ref[1] = author_out
    returned = jnp.dot(member_back, author_out, preferred_element_type=jnp.float32)
    result_ref[0] = (mid[core].astype(jnp.float32) + returned).astype(jnp.bfloat16)


def grid_kernel(
    count,
    partners_ref,
    tiles_hbm,
    feat_hbm,
    p_in_hbm,
    p_out_hbm,
    p_gain_ref,
    afeat_hbm,
    assign_ref,
    a_in_hbm,
    a_out_hbm,
    a_gain_ref,
    result_ref,
    w_p_in,
    w_p_out,
    w_a_in,
    w_a_out,
    tiles,
    plane_tiles,
    ring_tiles,
    ahead,
    back,
    mixed,
    linked,
    product,
    part_send,
    part_recv,
    pre,
    partial_send,
    partial_recv,
    afeat,
    apart_send,
    apart_recv,
    mid,
    author_pre,
    w_sem,
    load_sem,
    ring_send,
    ring_recv,
    tile_send,
    tile_recv,
    part_send_sem,
    part_recv_sem,
    core_send,
    core_recv,
):
    _, rows, width = afeat.shape
    half = rows // 2
    chunks = linked.shape[0]
    wide = width // chunks
    me = lax.axis_index("blk")
    core = lax.axis_index("auth")
    other = 1 - core
    slots = partners_ref.shape[1]
    z = me // PLANE
    y = lax.rem(me // 2, 2)
    x = lax.rem(me, 2)
    place = lax.rem(me, PLANE)

    def across(step):
        far_x = 1 - x if step % 2 else x
        far_y = 1 - y if step // 2 else y
        return far_y * 2 + far_x

    def level(step):
        return lax.rem(z + step, RING)

    def rows_of(index, size=rows):
        return pl.ds(pl.multiple_of(index * size, size), size)

    mine = rows_of(core, half)
    steps = range(1, PLANE)

    loads = [
        pltpu.make_async_copy(
            feat_hbm.at[:, n * wide : (n + 1) * wide],
            linked.at[n, rows_of(z)],
            load_sem.at[n],
        )
        for n in range(chunks)
    ]
    tile_load = pltpu.make_async_copy(tiles_hbm.at[0], tiles, load_sem.at[chunks])
    afeat_load = pltpu.make_async_copy(afeat_hbm, afeat.at[core], load_sem.at[chunks + 1])
    weights = [
        pltpu.make_async_copy(source, target, w_sem.at[slot])
        for slot, (source, target) in enumerate(
            ((p_in_hbm, w_p_in), (p_out_hbm, w_p_out), (a_in_hbm, w_a_in), (a_out_hbm, w_a_out))
        )
    ]

    barrier = pltpu.get_barrier_semaphore()
    for step in steps:
        for block in (z * PLANE + across(step), level(step) * PLANE + place):
            pl.semaphore_signal(barrier, inc=1, device_id={"blk": block}, device_id_type=MESH)
    pl.semaphore_signal(barrier, inc=1, device_id={"auth": other}, device_id_type=MESH)
    for load in loads:
        load.start()
    tile_load.start()
    afeat_load.start()

    def remote(source, target, send_sem, recv_sem, block):
        return pltpu.make_async_remote_copy(
            src_ref=source,
            dst_ref=target,
            send_sem=send_sem,
            recv_sem=recv_sem,
            device_id={"blk": block},
            device_id_type=MESH,
        )

    def arrived(target, semaphore):
        pltpu.make_async_copy(target, target, semaphore).wait()

    def to_core(source, target, slot):
        return to_other_core(source, target, core_send, core_recv, slot, other)

    even = 1 - lax.rem(z, 2)
    relay_from = lax.rem(z + 1 + 2 * even, RING)
    relay_to = lax.rem(z + 1 + 2 * (1 - even), RING)

    def ring_copy(kind, n):
        origin, target = (
            (z, level(1)),
            (z, level(RING - 1)),
            (relay_from, relay_to),
        )[kind]
        spot = linked.at[n, rows_of(origin)]
        return remote(
            spot,
            spot,
            ring_send.at[n * 3 + kind],
            ring_recv.at[n * RING + origin],
            target * PLANE + place,
        )

    def ring_arrived(n, origin):
        arrived(linked.at[n, rows_of(origin)], ring_recv.at[n * RING + origin])

    def plane_copy(step):
        return remote(
            plane_tiles.at[across(step), mine],
            ahead.at[place, mine],
            tile_send.at[step - 1],
            tile_recv.at[step - 1],
            z * PLANE + across(step),
        )

    def column_copy(step):
        return remote(
            ring_tiles.at[level(step), mine],
            back.at[z, mine],
            tile_send.at[PLANE + step - 1],
            tile_recv.at[PLANE + step - 1],
            level(step) * PLANE + place,
        )

    def part_copy(n, step):
        return remote(
            part_send.at[n, across(step)],
            part_recv.at[n, step - 1],
            part_send_sem.at[n * 3 + step - 1],
            part_recv_sem.at[n * 3 + step - 1],
            z * PLANE + across(step),
        )

    def start_own(n):
        ring_copy(0, n).start()
        ring_copy(1, n).start()

    def relay(n):
        ring_arrived(n, relay_from)
        ring_copy(2, n).start()

    for load in loads:
        load.wait()
    pl.semaphore_wait(barrier, 2 * (PLANE - 1) + 1)
    start_own(0)
    tile_load.wait()
    for block in range(count):
        index = jnp.int32(0)
        found = jnp.int32(0)
        for slot in range(slots):
            same = (partners_ref[0, slot] == block).astype(jnp.int32)
            index = jnp.maximum(index, same * slot)
            found = jnp.maximum(found, same)
        tile = tiles[index].astype(jnp.float32) * found.astype(jnp.float32)
        tile = tile.astype(jnp.bfloat16)
        upper, inner = block // PLANE, block % PLANE
        ring_tiles[upper, :, inner * rows : (inner + 1) * rows] = tile
        plane_tiles[inner, :, upper * rows : (upper + 1) * rows] = tile
    start_own(1)
    for step in (2, 1, 3):
        column_copy(step).start()
    for step in (3, 1, 2):
        plane_copy(step).start()
    for weight in weights:
        weight.start()
    afeat_load.wait()
    afeat_copy = to_core(afeat.at[core], afeat.at[core], 0)
    afeat_copy.start()

    relay(0)
    start_own(2)
    relay(1)
    start_own(3)

    ahead[place] = plane_tiles[place]
    plane_exchange = []
    for step in steps:
        spot = ahead.at[across(step), mine]
        arrived(spot, tile_recv.at[step - 1])
        copy = to_core(spot, spot, step)
        copy.start()
        plane_exchange.append(copy)
    column_exchange = []
    for step in steps:
        spot = back.at[level(RING - step), mine]
        arrived(spot, tile_recv.at[PLANE + step - 1])
        copy = to_core(spot, spot, PLANE - 1 + step)
        copy.start()
        column_exchange.append(copy)

    def mix(origin, came):
        columns = rows_of(origin)
        for inner in range(PLANE):
            own = ahead[inner, :, columns].astype(jnp.float32)
            there = came[origin, :, inner * rows : (inner + 1) * rows].astype(jnp.float32)
            mixed[inner * rows : (inner + 1) * rows, columns] = (own + there.T).astype(jnp.bfloat16)

    for copy in plane_exchange:
        copy.wait()
    mix(z, ring_tiles)
    for step in steps:
        column_exchange[step - 1].wait()
        mix(level(RING - step), back)

    def products(n):
        ring_arrived(n, relay_to)
        ring_arrived(n, level(2))
        total = jnp.dot(mixed[...], linked[n], preferred_element_type=jnp.float32)
        product[n] = total
        for inner in range(PLANE):
            part_send[n, inner] = total[inner * rows : (inner + 1) * rows].astype(jnp.bfloat16)
        for step in (3, 1, 2):
            part_copy(n, step).start()

    def collect(n):
        total = linked[n, rows_of(z)].astype(jnp.float32) + product[n, rows_of(place)]
        for step in steps:
            arrived(part_recv.at[n, step - 1], part_recv_sem.at[n * 3 + step - 1])
            total = total + part_recv[n, step - 1].astype(jnp.float32)
        spot = pre.at[core, :, n * wide : (n + 1) * wide]
        spot[...] = total.astype(jnp.bfloat16)
        copy = to_core(spot, spot, 2 * PLANE - 1 + n)
        copy.start()
        return copy

    def feed(side, start, stop):
        values = pre[side, :, start * wide : stop * wide].astype(jnp.float32)
        first = pl.multiple_of(side * width + start * wide, wide)
        columns = pl.ds(first, (stop - start) * wide)
        weighed = (values * p_gain_ref[:, columns]).astype(jnp.bfloat16)
        units = jnp.dot(weighed, w_p_in[columns, :], preferred_element_type=jnp.float32)
        return units, jnp.sum(values * values, axis=-1, keepdims=True)

    def add(units, square, more):
        return units + more[0], square + more[1]

    relay(2)
    products(0)
    products(1)
    relay(3)
    products(2)
    pre_copies = [collect(0), collect(1)]
    products(3)
    member_matrix, member_back, inverse = membership(assign_ref, afeat.shape[1], rows)
    weights[0].wait()
    units, square = feed(core, 0, 2)
    for copy in pre_copies:
        copy.wait()
    units, square = add(units, square, feed(other, 0, 2))
    for n in range(2, chunks):
        copy = collect(n)
        units, square = add(units, square, feed(core, n, n + 1))
        copy.wait()
        units, square = add(units, square, feed(other, n, n + 1))
    hidden = silu(units * lax.rsqrt(square / (2 * width) + epsilon))
    afeat_copy.wait()
    last = 2 * PLANE - 1 + chunks
    after_hidden(
        core,
        hidden,
        member_matrix,
        member_back,
        inverse,
        weights,
        to_core,
        (last, last + 1, last + 2),
        afeat,
        pre,
        w_p_out,
        w_a_in,
        w_a_out,
        a_gain_ref,
        partial_send,
        partial_recv,
        apart_send,
        apart_recv,
        mid,
        author_pre,
        result_ref,
    )

    for n in range(chunks):
        for kind in range(3):
            ring_copy(kind, n).wait_send()
        for step in steps:
            part_copy(n, step).wait_send()
    for step in steps:
        plane_copy(step).wait_send()
        column_copy(step).wait_send()


def direct_kernel(
    count,
    partners_ref,
    tiles_ref,
    feat_ref,
    p_in_hbm,
    p_out_hbm,
    p_gain_ref,
    afeat_ref,
    assign_ref,
    a_in_hbm,
    a_out_hbm,
    a_gain_ref,
    result_ref,
    w_p_in,
    w_p_out,
    w_a_in,
    w_a_out,
    dense,
    back,
    linked,
    mixed,
    pre,
    partial_send,
    partial_recv,
    afeat,
    apart_send,
    apart_recv,
    mid,
    author_pre,
    w_sem,
    relay_send,
    relay_recv,
    tile_send,
    tile_recv,
    core_send,
    core_recv,
):
    rows, width = feat_ref.shape
    half = rows // 2
    me = lax.axis_index("blk")
    core = lax.axis_index("auth")
    other = 1 - core
    slots = partners_ref.shape[1]

    weights = [
        pltpu.make_async_copy(source, target, w_sem.at[slot])
        for slot, (source, target) in enumerate(
            ((p_in_hbm, w_p_in), (p_out_hbm, w_p_out), (a_in_hbm, w_a_in), (a_out_hbm, w_a_out))
        )
    ]

    barrier = pltpu.get_barrier_semaphore()

    def greet(step, carry):
        block = lax.rem(me + step, count)
        pl.semaphore_signal(barrier, inc=1, device_id={"blk": block}, device_id_type=MESH)
        return carry

    lax.fori_loop(1, count, greet, 0)
    pl.semaphore_signal(barrier, inc=1, device_id={"auth": other}, device_id_type=MESH)

    def fill(block, carry):
        index = jnp.int32(0)
        found = jnp.int32(0)
        for slot in range(slots):
            same = (partners_ref[0, slot] == block).astype(jnp.int32)
            index = jnp.maximum(index, same * slot)
            found = jnp.maximum(found, same)
        tile = tiles_ref[0, index].astype(jnp.float32) * found.astype(jnp.float32)
        tile = tile.astype(jnp.bfloat16)
        dense[0, block] = tile[:half]
        dense[1, block] = tile[half:]
        return carry

    linked[pl.ds(pl.multiple_of(me * rows, rows), rows), :] = feat_ref[...]
    back[core, me] = jnp.zeros((half, rows), jnp.bfloat16)
    afeat[core] = afeat_ref[...]

    pl.semaphore_wait(barrier, count)

    def to_core(source, target, slot):
        return to_other_core(source, target, core_send, core_recv, slot, other)

    def tile_copy(step):
        block = lax.rem(me + step, count)
        return pltpu.make_async_remote_copy(
            src_ref=dense.at[core, block],
            dst_ref=back.at[core, me],
            send_sem=tile_send.at[step],
            recv_sem=tile_recv.at[step],
            device_id={"blk": block},
            device_id_type=MESH,
        )

    afeat_copy = to_core(afeat.at[core], afeat.at[core], 0)
    back_copy = to_core(back.at[core], back.at[core], 1)

    def direct(step):
        return pltpu.make_async_remote_copy(
            src_ref=feat_ref,
            dst_ref=linked.at[pl.ds(pl.multiple_of(me * rows, rows), rows)],
            send_sem=relay_send.at[step],
            recv_sem=relay_recv.at[step],
            device_id={"blk": lax.rem(me + step, count)},
            device_id_type=MESH,
        )

    def run(body):
        def one(step, carry):
            body(step)
            return carry

        lax.fori_loop(1, count, one, 0)

    run(lambda step: direct(step).start())
    lax.fori_loop(0, count, fill, 0)
    run(lambda step: tile_copy(step).start())
    afeat_copy.start()
    for weight in weights:
        weight.start()
    run(lambda step: tile_copy(step).wait())
    back_copy.start()
    back_copy.wait()

    def mix(block, carry):
        own = jnp.concatenate([dense[0, block], dense[1, block]], axis=0)
        came = jnp.concatenate([back[0, block], back[1, block]], axis=0)
        whole = own.astype(jnp.float32) + came.astype(jnp.float32).T
        mixed[:, pl.ds(pl.multiple_of(block * rows, rows), rows)] = whole.astype(jnp.bfloat16)
        return carry

    lax.fori_loop(0, count, mix, 0)
    run(lambda step: direct(step).wait())

    span = min(count * rows, 2048)

    def product(step, total):
        start = pl.multiple_of(step * span, span)
        return total + jnp.dot(
            mixed[:, pl.ds(start, span)],
            linked[pl.ds(start, span), :],
            preferred_element_type=jnp.float32,
        )

    total = feat_ref[...].astype(jnp.float32)
    total = lax.fori_loop(0, count * rows // span, product, total)
    pre[core] = total.astype(jnp.bfloat16)
    pre_copy = to_core(pre.at[core], pre.at[core], 2)
    pre_copy.start()

    member_matrix, member_back, inverse = membership(assign_ref, afeat_ref.shape[0], rows)
    weights[0].wait()
    own_units, own_square = scaled_units(pre, core, width, p_gain_ref, w_p_in)
    pre_copy.wait()
    far_units, far_square = scaled_units(pre, other, width, p_gain_ref, w_p_in)
    scale = lax.rsqrt((own_square + far_square) / (2 * width) + epsilon)
    hidden = silu((own_units + far_units) * scale)
    afeat_copy.wait()
    after_hidden(
        core,
        hidden,
        member_matrix,
        member_back,
        inverse,
        weights,
        to_core,
        (3, 4, 5),
        afeat,
        pre,
        w_p_out,
        w_a_in,
        w_a_out,
        a_gain_ref,
        partial_send,
        partial_recv,
        apart_send,
        apart_recv,
        mid,
        author_pre,
        result_ref,
    )


def local(
    features,
    partners,
    tiles,
    paper_w_in,
    paper_w_out,
    paper_gain,
    author_feats,
    assign,
    author_w_in,
    author_w_out,
    author_gain,
):
    count = lax.axis_size("blk")
    rows, width = features.shape
    bf16 = jnp.bfloat16
    f32 = jnp.float32
    vmem = pl.BlockSpec(memory_space=pltpu.VMEM)
    hbm = pl.BlockSpec(memory_space=pl.ANY)
    smem = pl.BlockSpec(memory_space=pltpu.SMEM)
    dma = pltpu.SemaphoreType.DMA
    pair = pltpu.VMEM((2, rows, width), bf16)
    single = pltpu.VMEM(author_feats.shape, bf16)
    held = [
        pltpu.VMEM(paper_w_in.shape, bf16),
        pltpu.VMEM(paper_w_out.shape, bf16),
        pltpu.VMEM(author_w_in.shape, bf16),
        pltpu.VMEM(author_w_out.shape, bf16),
    ]
    if count == PLANE * RING and width % LANES == 0:
        chunks = width // LANES
        body = grid_kernel
        near = hbm
        scratch = held + [
            pltpu.VMEM(tiles.shape[1:], bf16),
            pltpu.VMEM((PLANE, rows, RING * rows), bf16),
            pltpu.VMEM((RING, rows, PLANE * rows), bf16),
            pltpu.VMEM((PLANE, rows, RING * rows), bf16),
            pltpu.VMEM((RING, rows, PLANE * rows), bf16),
            pltpu.VMEM((PLANE * rows, RING * rows), bf16),
            pltpu.VMEM((chunks, RING * rows, LANES), bf16),
            pltpu.VMEM((chunks, PLANE * rows, LANES), f32),
            pltpu.VMEM((chunks, PLANE, rows, LANES), bf16),
            pltpu.VMEM((chunks, PLANE - 1, rows, LANES), bf16),
            pair,
            pair,
            pair,
            pair,
            single,
            single,
            pair,
            pair,
            dma((4,)),
            dma((chunks + 2,)),
            dma((chunks * 3,)),
            dma((chunks * RING,)),
            dma((PLANE + RING,)),
            dma((PLANE + RING,)),
            dma((chunks * (PLANE - 1),)),
            dma((chunks * (PLANE - 1),)),
            dma((2 * PLANE + 2 + chunks,)),
            dma((2 * PLANE + 2 + chunks,)),
        ]
    else:
        body = direct_kernel
        near = vmem
        tile_half = pltpu.VMEM((2, count, rows // 2, rows), bf16)
        scratch = held + [
            tile_half,
            tile_half,
            pltpu.VMEM((count * rows, width), bf16),
            pltpu.VMEM((rows, count * rows), bf16),
            pair,
            pair,
            pair,
            pair,
            single,
            single,
            pair,
            pair,
            dma((4,)),
            dma((count,)),
            dma((count,)),
            dma((count,)),
            dma((count,)),
            dma((6,)),
            dma((6,)),
        ]
    (result,) = pl.pallas_call(
        functools.partial(body, count),
        out_shape=(pltpu.VMEM((2,) + features.shape, bf16),),
        in_specs=[smem, near, near, hbm, hbm, vmem, near, vmem, hbm, hbm, vmem],
        out_specs=(vmem,),
        scratch_shapes=scratch,
        compiler_params=pltpu.CompilerParams(
            collective_id=0, has_side_effects=True, vmem_limit_bytes=56 * 1024 * 1024
        ),
    )(
        partners,
        tiles,
        features,
        paper_w_in,
        paper_w_out,
        paper_gain[None, :],
        author_feats,
        assign[None, :],
        author_w_in,
        author_w_out,
        author_gain[None, :],
    )
    return result[0], result[1]


def solution(mesh):
    placed = (
        P("blk", "auth"),
        P("blk", None),
        P("blk", None, None, None),
        P(None, "auth"),
        P("auth", None),
        P(),
        P("blk", "auth"),
        P("blk"),
        P(None, "auth"),
        P("auth", None),
        P(),
    )
    return jax.shard_map(
        local,
        mesh=mesh,
        in_specs=placed,
        out_specs=(P("blk", "auth"), P("blk", "auth")),
        check_vma=False,
    )
```

```python
import functools

import jax
import jax.numpy as jnp
from jax import lax
from jax.experimental import pallas as pl
from jax.experimental.pallas import tpu as pltpu
from jax.sharding import PartitionSpec as P

epsilon = 1e-06
MESH = pl.DeviceIdType.MESH
LANES = 128
PLANE = 4
RING = 4


def to_other_core(source, target, send_sem, recv_sem, slot, other):
    return pltpu.make_async_remote_copy(
        src_ref=source,
        dst_ref=target,
        send_sem=send_sem.at[slot],
        recv_sem=recv_sem.at[slot],
        device_id={"auth": other},
        device_id_type=MESH,
    )


def membership(assign_ref, authors, rows):
    member = assign_ref[...] == lax.broadcasted_iota(jnp.int32, (authors, rows), 0)
    member_wide = member.astype(jnp.float32)
    counts = jnp.maximum(jnp.sum(member_wide, axis=1, keepdims=True), 1.0)
    return member_wide.astype(jnp.bfloat16), member_wide.T.astype(jnp.bfloat16), 1.0 / counts


def silu(units):
    part = 0.5 * units
    return (part + part * jnp.tanh(part)).astype(jnp.bfloat16)


def scaled_units(pre, side, width, p_gain_ref, w_p_in):
    values = pre[side].astype(jnp.float32)
    columns = pl.ds(pl.multiple_of(side * width, width), width)
    weighed = (values * p_gain_ref[:, columns]).astype(jnp.bfloat16)
    units = jnp.dot(weighed, w_p_in[columns, :], preferred_element_type=jnp.float32)
    return units, jnp.sum(values * values, axis=-1, keepdims=True)


def after_hidden(
    core,
    hidden,
    member_matrix,
    member_back,
    inverse,
    weights,
    to_core,
    slots,
    afeat,
    pre,
    w_p_out,
    w_a_in,
    w_a_out,
    a_gain_ref,
    partial_send,
    partial_recv,
    apart_send,
    apart_recv,
    mid,
    author_pre,
    result_ref,
):
    other = 1 - core
    width = afeat.shape[2]
    weights[1].wait()
    terms = []
    partial_copies = []
    for side in range(2):
        term = jnp.dot(
            hidden,
            w_p_out[:, side * width : (side + 1) * width],
            preferred_element_type=jnp.float32,
        )
        terms.append(term)
        partial_send[side] = term.astype(jnp.bfloat16)
        copy = to_core(partial_send.at[side], partial_recv.at[side], slots[side])
        copy.start()
        partial_copies.append(copy)
    terms = [terms[side] + pre[side].astype(jnp.float32) for side in range(2)]
    weights[2].wait()
    units = 0.0
    square = 0.0
    for side in range(2):
        columns = slice(side * width, (side + 1) * width)
        partial_copies[side].wait()
        mid_side = (terms[side] + partial_recv[side].astype(jnp.float32)).astype(jnp.bfloat16)
        mid[side] = mid_side
        author_sum = jnp.dot(member_matrix, mid_side, preferred_element_type=jnp.float32)
        whole = (afeat[side].astype(jnp.float32) + author_sum * inverse).astype(jnp.bfloat16)
        author_pre[side] = whole
        values = whole.astype(jnp.float32)
        weighed = (values * a_gain_ref[:, columns]).astype(jnp.bfloat16)
        units = units + jnp.dot(weighed, w_a_in[columns, :], preferred_element_type=jnp.float32)
        square = square + jnp.sum(values * values, axis=-1, keepdims=True)
    hidden = silu(units * lax.rsqrt(square / (2 * width) + epsilon))
    weights[3].wait()
    theirs = pl.ds(pl.multiple_of(other * width, width), width)
    ours = pl.ds(pl.multiple_of(core * width, width), width)
    apart_send[...] = jnp.dot(
        hidden, w_a_out[:, theirs], preferred_element_type=jnp.float32
    ).astype(jnp.bfloat16)
    apart_copy = to_core(apart_send, apart_recv, slots[2])
    apart_copy.start()
    term = jnp.dot(hidden, w_a_out[:, ours], preferred_element_type=jnp.float32)
    term = term + author_pre[core].astype(jnp.float32)
    apart_copy.wait()
    author_out = (term + apart_recv[...].astype(jnp.float32)).astype(jnp.bfloat16)
    result_ref[1] = author_out
    returned = jnp.dot(member_back, author_out, preferred_element_type=jnp.float32)
    result_ref[0] = (mid[core].astype(jnp.float32) + returned).astype(jnp.bfloat16)


def grid_kernel(
    count,
    partners_ref,
    tiles_hbm,
    feat_hbm,
    p_in_hbm,
    p_out_hbm,
    p_gain_ref,
    afeat_hbm,
    assign_ref,
    a_in_hbm,
    a_out_hbm,
    a_gain_ref,
    result_ref,
    w_p_in,
    w_p_out,
    w_a_in,
    w_a_out,
    tiles,
    plane_tiles,
    ring_tiles,
    ahead,
    back,
    mixed,
    linked,
    product,
    part_send,
    part_recv,
    pre,
    partial_send,
    partial_recv,
    afeat,
    apart_send,
    apart_recv,
    mid,
    author_pre,
    w_sem,
    load_sem,
    ring_send,
    ring_recv,
    tile_send,
    tile_recv,
    part_send_sem,
    part_recv_sem,
    core_send,
    core_recv,
):
    _, rows, width = afeat.shape
    half = rows // 2
    chunks = linked.shape[0]
    wide = width // chunks
    me = lax.axis_index("blk")
    core = lax.axis_index("auth")
    other = 1 - core
    slots = partners_ref.shape[1]
    z = me // PLANE
    y = lax.rem(me // 2, 2)
    x = lax.rem(me, 2)
    place = lax.rem(me, PLANE)

    def across(step):
        far_x = 1 - x if step % 2 else x
        far_y = 1 - y if step // 2 else y
        return far_y * 2 + far_x

    def level(step):
        return lax.rem(z + step, RING)

    def rows_of(index, size=rows):
        return pl.ds(pl.multiple_of(index * size, size), size)

    mine = rows_of(core, half)
    steps = range(1, PLANE)

    loads = [
        pltpu.make_async_copy(
            feat_hbm.at[:, n * wide : (n + 1) * wide],
            linked.at[n, rows_of(z)],
            load_sem.at[n],
        )
        for n in range(chunks)
    ]
    tile_load = pltpu.make_async_copy(tiles_hbm.at[0], tiles, load_sem.at[chunks])
    afeat_load = pltpu.make_async_copy(afeat_hbm, afeat.at[core], load_sem.at[chunks + 1])
    weights = [
        pltpu.make_async_copy(source, target, w_sem.at[slot])
        for slot, (source, target) in enumerate(
            ((p_in_hbm, w_p_in), (p_out_hbm, w_p_out), (a_in_hbm, w_a_in), (a_out_hbm, w_a_out))
        )
    ]

    barrier = pltpu.get_barrier_semaphore()
    for step in steps:
        for block in (z * PLANE + across(step), level(step) * PLANE + place):
            pl.semaphore_signal(barrier, inc=1, device_id={"blk": block}, device_id_type=MESH)
    pl.semaphore_signal(barrier, inc=1, device_id={"auth": other}, device_id_type=MESH)
    for load in loads:
        load.start()
    tile_load.start()
    afeat_load.start()

    def remote(source, target, send_sem, recv_sem, block):
        return pltpu.make_async_remote_copy(
            src_ref=source,
            dst_ref=target,
            send_sem=send_sem,
            recv_sem=recv_sem,
            device_id={"blk": block},
            device_id_type=MESH,
        )

    def arrived(target, semaphore):
        pltpu.make_async_copy(target, target, semaphore).wait()

    def to_core(source, target, slot):
        return to_other_core(source, target, core_send, core_recv, slot, other)

    even = 1 - lax.rem(z, 2)
    relay_from = lax.rem(z + 1 + 2 * even, RING)
    relay_to = lax.rem(z + 1 + 2 * (1 - even), RING)

    def ring_copy(kind, n):
        origin, target = (
            (z, level(1)),
            (z, level(RING - 1)),
            (relay_from, relay_to),
        )[kind]
        spot = linked.at[n, rows_of(origin)]
        return remote(
            spot,
            spot,
            ring_send.at[n * 3 + kind],
            ring_recv.at[n * RING + origin],
            target * PLANE + place,
        )

    def ring_arrived(n, origin):
        arrived(linked.at[n, rows_of(origin)], ring_recv.at[n * RING + origin])

    def plane_copy(step):
        return remote(
            plane_tiles.at[across(step), mine],
            ahead.at[place, mine],
            tile_send.at[step - 1],
            tile_recv.at[step - 1],
            z * PLANE + across(step),
        )

    def column_copy(step):
        return remote(
            ring_tiles.at[level(step), mine],
            back.at[z, mine],
            tile_send.at[PLANE + step - 1],
            tile_recv.at[PLANE + step - 1],
            level(step) * PLANE + place,
        )

    def part_copy(n, step):
        return remote(
            part_send.at[n, across(step)],
            part_recv.at[n, step - 1],
            part_send_sem.at[n * 3 + step - 1],
            part_recv_sem.at[n * 3 + step - 1],
            z * PLANE + across(step),
        )

    def start_own(n):
        ring_copy(0, n).start()
        ring_copy(1, n).start()

    def relay(n):
        ring_arrived(n, relay_from)
        ring_copy(2, n).start()

    for load in loads:
        load.wait()
    pl.semaphore_wait(barrier, 2 * (PLANE - 1) + 1)
    start_own(0)
    tile_load.wait()
    for block in range(count):
        index = jnp.int32(0)
        found = jnp.int32(0)
        for slot in range(slots):
            same = (partners_ref[0, slot] == block).astype(jnp.int32)
            index = jnp.maximum(index, same * slot)
            found = jnp.maximum(found, same)
        tile = tiles[index].astype(jnp.float32) * found.astype(jnp.float32)
        tile = tile.astype(jnp.bfloat16)
        upper, inner = block // PLANE, block % PLANE
        ring_tiles[upper, :, inner * rows : (inner + 1) * rows] = tile
        plane_tiles[inner, :, upper * rows : (upper + 1) * rows] = tile
    start_own(1)
    for step in (2, 1, 3):
        column_copy(step).start()
    for step in (3, 1, 2):
        plane_copy(step).start()
    for weight in weights:
        weight.start()
    afeat_load.wait()
    afeat_copy = to_core(afeat.at[core], afeat.at[core], 0)
    afeat_copy.start()

    start_own(2)
    relay(0)
    relay(1)
    start_own(3)

    ahead[place] = plane_tiles[place]
    plane_exchange = []
    for step in steps:
        spot = ahead.at[across(step), mine]
        arrived(spot, tile_recv.at[step - 1])
        copy = to_core(spot, spot, step)
        copy.start()
        plane_exchange.append(copy)
    column_exchange = []
    for step in steps:
        spot = back.at[level(RING - step), mine]
        arrived(spot, tile_recv.at[PLANE + step - 1])
        copy = to_core(spot, spot, PLANE - 1 + step)
        copy.start()
        column_exchange.append(copy)

    def mix(origin, came):
        columns = rows_of(origin)
        for inner in range(PLANE):
            own = ahead[inner, :, columns].astype(jnp.float32)
            there = came[origin, :, inner * rows : (inner + 1) * rows].astype(jnp.float32)
            mixed[inner * rows : (inner + 1) * rows, columns] = (own + there.T).astype(jnp.bfloat16)

    for copy in plane_exchange:
        copy.wait()
    mix(z, ring_tiles)
    relay(2)
    for step in steps:
        column_exchange[step - 1].wait()
        mix(level(RING - step), back)

    def products(n):
        ring_arrived(n, relay_to)
        ring_arrived(n, level(2))
        total = jnp.dot(mixed[...], linked[n], preferred_element_type=jnp.float32)
        product[n] = total
        for inner in range(PLANE):
            part_send[n, inner] = total[inner * rows : (inner + 1) * rows].astype(jnp.bfloat16)
        for step in (3, 1, 2):
            part_copy(n, step).start()

    def collect(n):
        total = linked[n, rows_of(z)].astype(jnp.float32) + product[n, rows_of(place)]
        for step in steps:
            arrived(part_recv.at[n, step - 1], part_recv_sem.at[n * 3 + step - 1])
            total = total + part_recv[n, step - 1].astype(jnp.float32)
        spot = pre.at[core, :, n * wide : (n + 1) * wide]
        spot[...] = total.astype(jnp.bfloat16)
        copy = to_core(spot, spot, 2 * PLANE - 1 + n)
        copy.start()
        return copy

    def feed(side, start, stop):
        values = pre[side, :, start * wide : stop * wide].astype(jnp.float32)
        first = pl.multiple_of(side * width + start * wide, wide)
        columns = pl.ds(first, (stop - start) * wide)
        weighed = (values * p_gain_ref[:, columns]).astype(jnp.bfloat16)
        units = jnp.dot(weighed, w_p_in[columns, :], preferred_element_type=jnp.float32)
        return units, jnp.sum(values * values, axis=-1, keepdims=True)

    def add(units, square, more):
        return units + more[0], square + more[1]

    products(0)
    products(1)
    relay(3)
    products(2)
    products(3)
    pre_copies = [collect(0), collect(1)]
    member_matrix, member_back, inverse = membership(assign_ref, afeat.shape[1], rows)
    weights[0].wait()
    units, square = feed(core, 0, 2)
    for copy in pre_copies:
        copy.wait()
    units, square = add(units, square, feed(other, 0, 2))
    for n in range(2, chunks):
        copy = collect(n)
        units, square = add(units, square, feed(core, n, n + 1))
        copy.wait()
        units, square = add(units, square, feed(other, n, n + 1))
    hidden = silu(units * lax.rsqrt(square / (2 * width) + epsilon))
    afeat_copy.wait()
    last = 2 * PLANE - 1 + chunks
    after_hidden(
        core,
        hidden,
        member_matrix,
        member_back,
        inverse,
        weights,
        to_core,
        (last, last + 1, last + 2),
        afeat,
        pre,
        w_p_out,
        w_a_in,
        w_a_out,
        a_gain_ref,
        partial_send,
        partial_recv,
        apart_send,
        apart_recv,
        mid,
        author_pre,
        result_ref,
    )

    for n in range(chunks):
        for kind in range(3):
            ring_copy(kind, n).wait_send()
        for step in steps:
            part_copy(n, step).wait_send()
    for step in steps:
        plane_copy(step).wait_send()
        column_copy(step).wait_send()


def direct_kernel(
    count,
    partners_ref,
    tiles_ref,
    feat_ref,
    p_in_hbm,
    p_out_hbm,
    p_gain_ref,
    afeat_ref,
    assign_ref,
    a_in_hbm,
    a_out_hbm,
    a_gain_ref,
    result_ref,
    w_p_in,
    w_p_out,
    w_a_in,
    w_a_out,
    dense,
    back,
    linked,
    mixed,
    pre,
    partial_send,
    partial_recv,
    afeat,
    apart_send,
    apart_recv,
    mid,
    author_pre,
    w_sem,
    relay_send,
    relay_recv,
    tile_send,
    tile_recv,
    core_send,
    core_recv,
):
    rows, width = feat_ref.shape
    half = rows // 2
    me = lax.axis_index("blk")
    core = lax.axis_index("auth")
    other = 1 - core
    slots = partners_ref.shape[1]

    weights = [
        pltpu.make_async_copy(source, target, w_sem.at[slot])
        for slot, (source, target) in enumerate(
            ((p_in_hbm, w_p_in), (p_out_hbm, w_p_out), (a_in_hbm, w_a_in), (a_out_hbm, w_a_out))
        )
    ]

    barrier = pltpu.get_barrier_semaphore()

    def greet(step, carry):
        block = lax.rem(me + step, count)
        pl.semaphore_signal(barrier, inc=1, device_id={"blk": block}, device_id_type=MESH)
        return carry

    lax.fori_loop(1, count, greet, 0)
    pl.semaphore_signal(barrier, inc=1, device_id={"auth": other}, device_id_type=MESH)

    def fill(block, carry):
        index = jnp.int32(0)
        found = jnp.int32(0)
        for slot in range(slots):
            same = (partners_ref[0, slot] == block).astype(jnp.int32)
            index = jnp.maximum(index, same * slot)
            found = jnp.maximum(found, same)
        tile = tiles_ref[0, index].astype(jnp.float32) * found.astype(jnp.float32)
        tile = tile.astype(jnp.bfloat16)
        dense[0, block] = tile[:half]
        dense[1, block] = tile[half:]
        return carry

    linked[pl.ds(pl.multiple_of(me * rows, rows), rows), :] = feat_ref[...]
    back[core, me] = jnp.zeros((half, rows), jnp.bfloat16)
    afeat[core] = afeat_ref[...]

    pl.semaphore_wait(barrier, count)

    def to_core(source, target, slot):
        return to_other_core(source, target, core_send, core_recv, slot, other)

    def tile_copy(step):
        block = lax.rem(me + step, count)
        return pltpu.make_async_remote_copy(
            src_ref=dense.at[core, block],
            dst_ref=back.at[core, me],
            send_sem=tile_send.at[step],
            recv_sem=tile_recv.at[step],
            device_id={"blk": block},
            device_id_type=MESH,
        )

    afeat_copy = to_core(afeat.at[core], afeat.at[core], 0)
    back_copy = to_core(back.at[core], back.at[core], 1)

    def direct(step):
        return pltpu.make_async_remote_copy(
            src_ref=feat_ref,
            dst_ref=linked.at[pl.ds(pl.multiple_of(me * rows, rows), rows)],
            send_sem=relay_send.at[step],
            recv_sem=relay_recv.at[step],
            device_id={"blk": lax.rem(me + step, count)},
            device_id_type=MESH,
        )

    def run(body):
        def one(step, carry):
            body(step)
            return carry

        lax.fori_loop(1, count, one, 0)

    run(lambda step: direct(step).start())
    lax.fori_loop(0, count, fill, 0)
    run(lambda step: tile_copy(step).start())
    afeat_copy.start()
    for weight in weights:
        weight.start()
    run(lambda step: tile_copy(step).wait())
    back_copy.start()
    back_copy.wait()

    def mix(block, carry):
        own = jnp.concatenate([dense[0, block], dense[1, block]], axis=0)
        came = jnp.concatenate([back[0, block], back[1, block]], axis=0)
        whole = own.astype(jnp.float32) + came.astype(jnp.float32).T
        mixed[:, pl.ds(pl.multiple_of(block * rows, rows), rows)] = whole.astype(jnp.bfloat16)
        return carry

    lax.fori_loop(0, count, mix, 0)
    run(lambda step: direct(step).wait())

    span = min(count * rows, 2048)

    def product(step, total):
        start = pl.multiple_of(step * span, span)
        return total + jnp.dot(
            mixed[:, pl.ds(start, span)],
            linked[pl.ds(start, span), :],
            preferred_element_type=jnp.float32,
        )

    total = feat_ref[...].astype(jnp.float32)
    total = lax.fori_loop(0, count * rows // span, product, total)
    pre[core] = total.astype(jnp.bfloat16)
    pre_copy = to_core(pre.at[core], pre.at[core], 2)
    pre_copy.start()

    member_matrix, member_back, inverse = membership(assign_ref, afeat_ref.shape[0], rows)
    weights[0].wait()
    own_units, own_square = scaled_units(pre, core, width, p_gain_ref, w_p_in)
    pre_copy.wait()
    far_units, far_square = scaled_units(pre, other, width, p_gain_ref, w_p_in)
    scale = lax.rsqrt((own_square + far_square) / (2 * width) + epsilon)
    hidden = silu((own_units + far_units) * scale)
    afeat_copy.wait()
    after_hidden(
        core,
        hidden,
        member_matrix,
        member_back,
        inverse,
        weights,
        to_core,
        (3, 4, 5),
        afeat,
        pre,
        w_p_out,
        w_a_in,
        w_a_out,
        a_gain_ref,
        partial_send,
        partial_recv,
        apart_send,
        apart_recv,
        mid,
        author_pre,
        result_ref,
    )


def local(
    features,
    partners,
    tiles,
    paper_w_in,
    paper_w_out,
    paper_gain,
    author_feats,
    assign,
    author_w_in,
    author_w_out,
    author_gain,
):
    count = lax.axis_size("blk")
    rows, width = features.shape
    bf16 = jnp.bfloat16
    f32 = jnp.float32
    vmem = pl.BlockSpec(memory_space=pltpu.VMEM)
    hbm = pl.BlockSpec(memory_space=pl.ANY)
    smem = pl.BlockSpec(memory_space=pltpu.SMEM)
    dma = pltpu.SemaphoreType.DMA
    pair = pltpu.VMEM((2, rows, width), bf16)
    single = pltpu.VMEM(author_feats.shape, bf16)
    held = [
        pltpu.VMEM(paper_w_in.shape, bf16),
        pltpu.VMEM(paper_w_out.shape, bf16),
        pltpu.VMEM(author_w_in.shape, bf16),
        pltpu.VMEM(author_w_out.shape, bf16),
    ]
    if count == PLANE * RING and width % LANES == 0:
        chunks = width // LANES
        body = grid_kernel
        near = hbm
        scratch = held + [
            pltpu.VMEM(tiles.shape[1:], bf16),
            pltpu.VMEM((PLANE, rows, RING * rows), bf16),
            pltpu.VMEM((RING, rows, PLANE * rows), bf16),
            pltpu.VMEM((PLANE, rows, RING * rows), bf16),
            pltpu.VMEM((RING, rows, PLANE * rows), bf16),
            pltpu.VMEM((PLANE * rows, RING * rows), bf16),
            pltpu.VMEM((chunks, RING * rows, LANES), bf16),
            pltpu.VMEM((chunks, PLANE * rows, LANES), f32),
            pltpu.VMEM((chunks, PLANE, rows, LANES), bf16),
            pltpu.VMEM((chunks, PLANE - 1, rows, LANES), bf16),
            pair,
            pair,
            pair,
            pair,
            single,
            single,
            pair,
            pair,
            dma((4,)),
            dma((chunks + 2,)),
            dma((chunks * 3,)),
            dma((chunks * RING,)),
            dma((PLANE + RING,)),
            dma((PLANE + RING,)),
            dma((chunks * (PLANE - 1),)),
            dma((chunks * (PLANE - 1),)),
            dma((2 * PLANE + 2 + chunks,)),
            dma((2 * PLANE + 2 + chunks,)),
        ]
    else:
        body = direct_kernel
        near = vmem
        tile_half = pltpu.VMEM((2, count, rows // 2, rows), bf16)
        scratch = held + [
            tile_half,
            tile_half,
            pltpu.VMEM((count * rows, width), bf16),
            pltpu.VMEM((rows, count * rows), bf16),
            pair,
            pair,
            pair,
            pair,
            single,
            single,
            pair,
            pair,
            dma((4,)),
            dma((count,)),
            dma((count,)),
            dma((count,)),
            dma((count,)),
            dma((6,)),
            dma((6,)),
        ]
    (result,) = pl.pallas_call(
        functools.partial(body, count),
        out_shape=(pltpu.VMEM((2,) + features.shape, bf16),),
        in_specs=[smem, near, near, hbm, hbm, vmem, near, vmem, hbm, hbm, vmem],
        out_specs=(vmem,),
        scratch_shapes=scratch,
        compiler_params=pltpu.CompilerParams(
            collective_id=0, has_side_effects=True, vmem_limit_bytes=56 * 1024 * 1024
        ),
    )(
        partners,
        tiles,
        features,
        paper_w_in,
        paper_w_out,
        paper_gain[None, :],
        author_feats,
        assign[None, :],
        author_w_in,
        author_w_out,
        author_gain[None, :],
    )
    return result[0], result[1]


def solution(mesh):
    placed = (
        P("blk", "auth"),
        P("blk", None),
        P("blk", None, None, None),
        P(None, "auth"),
        P("auth", None),
        P(),
        P("blk", "auth"),
        P("blk"),
        P(None, "auth"),
        P("auth", None),
        P(),
    )
    return jax.shard_map(
        local,
        mesh=mesh,
        in_specs=placed,
        out_specs=(P("blk", "auth"), P("blk", "auth")),
        check_vma=False,
    )
```

```python
import functools

import jax
import jax.numpy as jnp
from jax import lax
from jax.experimental import pallas as pl
from jax.experimental.pallas import tpu as pltpu
from jax.sharding import PartitionSpec as P

epsilon = 1e-06
MESH = pl.DeviceIdType.MESH
LANES = 128
PLANE = 4
RING = 4


def to_other_core(source, target, send_sem, recv_sem, slot, other):
    return pltpu.make_async_remote_copy(
        src_ref=source,
        dst_ref=target,
        send_sem=send_sem.at[slot],
        recv_sem=recv_sem.at[slot],
        device_id={"auth": other},
        device_id_type=MESH,
    )


def membership(assign_ref, authors, rows):
    member = assign_ref[...] == lax.broadcasted_iota(jnp.int32, (authors, rows), 0)
    member_wide = member.astype(jnp.float32)
    counts = jnp.maximum(jnp.sum(member_wide, axis=1, keepdims=True), 1.0)
    return member_wide.astype(jnp.bfloat16), member_wide.T.astype(jnp.bfloat16), 1.0 / counts


def silu(units):
    part = 0.5 * units
    return (part + part * jnp.tanh(part)).astype(jnp.bfloat16)


def hidden_of(units, weighed, w_in, columns, scale):
    span = 2 * LANES
    parts = []
    for start in range(0, w_in.shape[1], span):
        more = jnp.dot(
            weighed,
            w_in[columns, start : start + span],
            preferred_element_type=jnp.float32,
        )
        parts.append(silu((units[:, start : start + span] + more) * scale))
    return jnp.concatenate(parts, axis=1)


def scaled_units(pre, side, width, p_gain_ref, w_p_in):
    values = pre[side].astype(jnp.float32)
    columns = pl.ds(pl.multiple_of(side * width, width), width)
    weighed = (values * p_gain_ref[:, columns]).astype(jnp.bfloat16)
    units = jnp.dot(weighed, w_p_in[columns, :], preferred_element_type=jnp.float32)
    return units, jnp.sum(values * values, axis=-1, keepdims=True)


def after_hidden(
    core,
    hidden,
    member_matrix,
    member_back,
    inverse,
    weights,
    to_core,
    slots,
    afeat,
    pre,
    w_p_out,
    w_a_in,
    w_a_out,
    a_gain_ref,
    partial_send,
    partial_recv,
    apart_send,
    apart_recv,
    mid,
    author_pre,
    result_ref,
):
    other = 1 - core
    width = afeat.shape[2]
    weights[1].wait()
    terms = []
    partial_copies = []
    for side in range(2):
        term = jnp.dot(
            hidden,
            w_p_out[:, side * width : (side + 1) * width],
            preferred_element_type=jnp.float32,
        )
        terms.append(term)
        partial_send[side] = term.astype(jnp.bfloat16)
        copy = to_core(partial_send.at[side], partial_recv.at[side], slots[side])
        copy.start()
        partial_copies.append(copy)
    terms = [terms[side] + pre[side].astype(jnp.float32) for side in range(2)]
    weights[2].wait()
    square = 0.0
    for side in range(2):
        columns = slice(side * width, (side + 1) * width)
        partial_copies[side].wait()
        mid_side = (terms[side] + partial_recv[side].astype(jnp.float32)).astype(jnp.bfloat16)
        mid[side] = mid_side
        author_sum = jnp.dot(member_matrix, mid_side, preferred_element_type=jnp.float32)
        whole = (afeat[side].astype(jnp.float32) + author_sum * inverse).astype(jnp.bfloat16)
        author_pre[side] = whole
        values = whole.astype(jnp.float32)
        weighed = (values * a_gain_ref[:, columns]).astype(jnp.bfloat16)
        square = square + jnp.sum(values * values, axis=-1, keepdims=True)
        if side == 0:
            units = jnp.dot(weighed, w_a_in[columns, :], preferred_element_type=jnp.float32)
    scale = lax.rsqrt(square / (2 * width) + epsilon)
    hidden = hidden_of(units, weighed, w_a_in, columns, scale)
    weights[3].wait()
    theirs = pl.ds(pl.multiple_of(other * width, width), width)
    ours = pl.ds(pl.multiple_of(core * width, width), width)
    apart_send[...] = jnp.dot(
        hidden, w_a_out[:, theirs], preferred_element_type=jnp.float32
    ).astype(jnp.bfloat16)
    apart_copy = to_core(apart_send, apart_recv, slots[2])
    apart_copy.start()
    term = jnp.dot(hidden, w_a_out[:, ours], preferred_element_type=jnp.float32)
    term = term + author_pre[core].astype(jnp.float32)
    apart_copy.wait()
    author_out = (term + apart_recv[...].astype(jnp.float32)).astype(jnp.bfloat16)
    result_ref[1] = author_out
    returned = jnp.dot(member_back, author_out, preferred_element_type=jnp.float32)
    result_ref[0] = (mid[core].astype(jnp.float32) + returned).astype(jnp.bfloat16)


def grid_kernel(
    count,
    partners_ref,
    tiles_hbm,
    feat_hbm,
    p_in_hbm,
    p_out_hbm,
    p_gain_ref,
    afeat_hbm,
    assign_ref,
    a_in_hbm,
    a_out_hbm,
    a_gain_ref,
    result_ref,
    w_p_in,
    w_p_out,
    w_a_in,
    w_a_out,
    tiles,
    plane_tiles,
    ring_tiles,
    ahead,
    back,
    mixed,
    linked,
    product,
    part_send,
    part_recv,
    pre,
    partial_send,
    partial_recv,
    afeat,
    apart_send,
    apart_recv,
    mid,
    author_pre,
    w_sem,
    load_sem,
    ring_send,
    ring_recv,
    tile_send,
    tile_recv,
    part_send_sem,
    part_recv_sem,
    core_send,
    core_recv,
):
    _, rows, width = afeat.shape
    half = rows // 2
    chunks = linked.shape[0]
    wide = width // chunks
    me = lax.axis_index("blk")
    core = lax.axis_index("auth")
    other = 1 - core
    slots = partners_ref.shape[1]
    z = me // PLANE
    y = lax.rem(me // 2, 2)
    x = lax.rem(me, 2)
    place = lax.rem(me, PLANE)

    def across(step):
        far_x = 1 - x if step % 2 else x
        far_y = 1 - y if step // 2 else y
        return far_y * 2 + far_x

    def level(step):
        return lax.rem(z + step, RING)

    def rows_of(index, size=rows):
        return pl.ds(pl.multiple_of(index * size, size), size)

    mine = rows_of(core, half)
    steps = range(1, PLANE)

    loads = [
        pltpu.make_async_copy(
            feat_hbm.at[:, n * wide : (n + 1) * wide],
            linked.at[n, rows_of(z)],
            load_sem.at[n],
        )
        for n in range(chunks)
    ]
    tile_load = pltpu.make_async_copy(tiles_hbm.at[0], tiles, load_sem.at[chunks])
    afeat_load = pltpu.make_async_copy(afeat_hbm, afeat.at[core], load_sem.at[chunks + 1])
    weights = [
        pltpu.make_async_copy(source, target, w_sem.at[slot])
        for slot, (source, target) in enumerate(
            ((p_in_hbm, w_p_in), (p_out_hbm, w_p_out), (a_in_hbm, w_a_in), (a_out_hbm, w_a_out))
        )
    ]

    barrier = pltpu.get_barrier_semaphore()
    for step in steps:
        for block in (z * PLANE + across(step), level(step) * PLANE + place):
            pl.semaphore_signal(barrier, inc=1, device_id={"blk": block}, device_id_type=MESH)
    pl.semaphore_signal(barrier, inc=1, device_id={"auth": other}, device_id_type=MESH)
    for load in loads:
        load.start()
    tile_load.start()
    afeat_load.start()

    def remote(source, target, send_sem, recv_sem, block):
        return pltpu.make_async_remote_copy(
            src_ref=source,
            dst_ref=target,
            send_sem=send_sem,
            recv_sem=recv_sem,
            device_id={"blk": block},
            device_id_type=MESH,
        )

    def arrived(target, semaphore):
        pltpu.make_async_copy(target, target, semaphore).wait()

    def to_core(source, target, slot):
        return to_other_core(source, target, core_send, core_recv, slot, other)

    even = 1 - lax.rem(z, 2)
    relay_from = lax.rem(z + 1 + 2 * even, RING)
    relay_to = lax.rem(z + 1 + 2 * (1 - even), RING)

    def ring_copy(kind, n):
        origin, target = (
            (z, level(1)),
            (z, level(RING - 1)),
            (relay_from, relay_to),
        )[kind]
        spot = linked.at[n, rows_of(origin)]
        return remote(
            spot,
            spot,
            ring_send.at[n * 3 + kind],
            ring_recv.at[n * RING + origin],
            target * PLANE + place,
        )

    def ring_arrived(n, origin):
        arrived(linked.at[n, rows_of(origin)], ring_recv.at[n * RING + origin])

    def plane_copy(step):
        return remote(
            plane_tiles.at[across(step), mine],
            ahead.at[place, mine],
            tile_send.at[step - 1],
            tile_recv.at[step - 1],
            z * PLANE + across(step),
        )

    def column_copy(step):
        return remote(
            ring_tiles.at[level(step), mine],
            back.at[z, mine],
            tile_send.at[PLANE + step - 1],
            tile_recv.at[PLANE + step - 1],
            level(step) * PLANE + place,
        )

    def part_copy(n, step):
        return remote(
            part_send.at[n, across(step)],
            part_recv.at[n, step - 1],
            part_send_sem.at[n * 3 + step - 1],
            part_recv_sem.at[n * 3 + step - 1],
            z * PLANE + across(step),
        )

    def start_own(n):
        ring_copy(0, n).start()
        ring_copy(1, n).start()

    def relay(n):
        ring_arrived(n, relay_from)
        ring_copy(2, n).start()

    for load in loads:
        load.wait()
    pl.semaphore_wait(barrier, 2 * (PLANE - 1) + 1)
    start_own(0)
    tile_load.wait()
    for block in range(count):
        index = jnp.int32(0)
        found = jnp.int32(0)
        for slot in range(slots):
            same = (partners_ref[0, slot] == block).astype(jnp.int32)
            index = jnp.maximum(index, same * slot)
            found = jnp.maximum(found, same)
        tile = tiles[index].astype(jnp.float32) * found.astype(jnp.float32)
        tile = tile.astype(jnp.bfloat16)
        upper, inner = block // PLANE, block % PLANE
        ring_tiles[upper, :, inner * rows : (inner + 1) * rows] = tile
        plane_tiles[inner, :, upper * rows : (upper + 1) * rows] = tile
    start_own(1)
    for step in (2, 1, 3):
        column_copy(step).start()
    for step in (3, 1, 2):
        plane_copy(step).start()
    for weight in weights:
        weight.start()
    afeat_load.wait()
    afeat_copy = to_core(afeat.at[core], afeat.at[core], 0)
    afeat_copy.start()

    start_own(2)
    relay(0)
    relay(1)
    start_own(3)

    ahead[place] = plane_tiles[place]
    plane_exchange = []
    for step in steps:
        spot = ahead.at[across(step), mine]
        arrived(spot, tile_recv.at[step - 1])
        copy = to_core(spot, spot, step)
        copy.start()
        plane_exchange.append(copy)
    column_exchange = []
    for step in steps:
        spot = back.at[level(RING - step), mine]
        arrived(spot, tile_recv.at[PLANE + step - 1])
        copy = to_core(spot, spot, PLANE - 1 + step)
        copy.start()
        column_exchange.append(copy)

    def mix(origin, came):
        columns = rows_of(origin)
        for inner in range(PLANE):
            own = ahead[inner, :, columns].astype(jnp.float32)
            there = came[origin, :, inner * rows : (inner + 1) * rows].astype(jnp.float32)
            mixed[inner * rows : (inner + 1) * rows, columns] = (own + there.T).astype(jnp.bfloat16)

    for copy in plane_exchange:
        copy.wait()
    mix(z, ring_tiles)
    relay(2)
    for step in steps:
        column_exchange[step - 1].wait()
        mix(level(RING - step), back)

    def products(n):
        ring_arrived(n, relay_to)
        ring_arrived(n, level(2))
        total = jnp.dot(mixed[...], linked[n], preferred_element_type=jnp.float32)
        product[n] = total
        for inner in range(PLANE):
            part_send[n, inner] = total[inner * rows : (inner + 1) * rows].astype(jnp.bfloat16)
        for step in (3, 1, 2):
            part_copy(n, step).start()

    def collect(n):
        total = linked[n, rows_of(z)].astype(jnp.float32) + product[n, rows_of(place)]
        for step in steps:
            arrived(part_recv.at[n, step - 1], part_recv_sem.at[n * 3 + step - 1])
            total = total + part_recv[n, step - 1].astype(jnp.float32)
        spot = pre.at[core, :, n * wide : (n + 1) * wide]
        spot[...] = total.astype(jnp.bfloat16)
        copy = to_core(spot, spot, 2 * PLANE - 1 + n)
        copy.start()
        return copy

    def weigh(side, start, stop):
        values = pre[side, :, start * wide : stop * wide].astype(jnp.float32)
        first = pl.multiple_of(side * width + start * wide, wide)
        columns = pl.ds(first, (stop - start) * wide)
        weighed = (values * p_gain_ref[:, columns]).astype(jnp.bfloat16)
        return weighed, columns, jnp.sum(values * values, axis=-1, keepdims=True)

    def feed(side, start, stop):
        weighed, columns, square = weigh(side, start, stop)
        units = jnp.dot(weighed, w_p_in[columns, :], preferred_element_type=jnp.float32)
        return units, square

    def add(units, square, more):
        return units + more[0], square + more[1]

    products(0)
    products(1)
    relay(3)
    products(2)
    products(3)
    pre_copies = [collect(0), collect(1)]
    member_matrix, member_back, inverse = membership(assign_ref, afeat.shape[1], rows)
    weights[0].wait()
    units, square = feed(core, 0, 2)
    for copy in pre_copies:
        copy.wait()
    units, square = add(units, square, feed(other, 0, 2))
    for n in range(2, chunks):
        copy = collect(n)
        units, square = add(units, square, feed(core, n, n + 1))
        copy.wait()
        if n < chunks - 1:
            units, square = add(units, square, feed(other, n, n + 1))
    weighed, columns, more = weigh(other, chunks - 1, chunks)
    scale = lax.rsqrt((square + more) / (2 * width) + epsilon)
    hidden = hidden_of(units, weighed, w_p_in, columns, scale)
    afeat_copy.wait()
    last = 2 * PLANE - 1 + chunks
    after_hidden(
        core,
        hidden,
        member_matrix,
        member_back,
        inverse,
        weights,
        to_core,
        (last, last + 1, last + 2),
        afeat,
        pre,
        w_p_out,
        w_a_in,
        w_a_out,
        a_gain_ref,
        partial_send,
        partial_recv,
        apart_send,
        apart_recv,
        mid,
        author_pre,
        result_ref,
    )

    for n in range(chunks):
        for kind in range(3):
            ring_copy(kind, n).wait_send()
        for step in steps:
            part_copy(n, step).wait_send()
    for step in steps:
        plane_copy(step).wait_send()
        column_copy(step).wait_send()


def direct_kernel(
    count,
    partners_ref,
    tiles_ref,
    feat_ref,
    p_in_hbm,
    p_out_hbm,
    p_gain_ref,
    afeat_ref,
    assign_ref,
    a_in_hbm,
    a_out_hbm,
    a_gain_ref,
    result_ref,
    w_p_in,
    w_p_out,
    w_a_in,
    w_a_out,
    dense,
    back,
    linked,
    mixed,
    pre,
    partial_send,
    partial_recv,
    afeat,
    apart_send,
    apart_recv,
    mid,
    author_pre,
    w_sem,
    relay_send,
    relay_recv,
    tile_send,
    tile_recv,
    core_send,
    core_recv,
):
    rows, width = feat_ref.shape
    half = rows // 2
    me = lax.axis_index("blk")
    core = lax.axis_index("auth")
    other = 1 - core
    slots = partners_ref.shape[1]

    weights = [
        pltpu.make_async_copy(source, target, w_sem.at[slot])
        for slot, (source, target) in enumerate(
            ((p_in_hbm, w_p_in), (p_out_hbm, w_p_out), (a_in_hbm, w_a_in), (a_out_hbm, w_a_out))
        )
    ]

    barrier = pltpu.get_barrier_semaphore()

    def greet(step, carry):
        block = lax.rem(me + step, count)
        pl.semaphore_signal(barrier, inc=1, device_id={"blk": block}, device_id_type=MESH)
        return carry

    lax.fori_loop(1, count, greet, 0)
    pl.semaphore_signal(barrier, inc=1, device_id={"auth": other}, device_id_type=MESH)

    def fill(block, carry):
        index = jnp.int32(0)
        found = jnp.int32(0)
        for slot in range(slots):
            same = (partners_ref[0, slot] == block).astype(jnp.int32)
            index = jnp.maximum(index, same * slot)
            found = jnp.maximum(found, same)
        tile = tiles_ref[0, index].astype(jnp.float32) * found.astype(jnp.float32)
        tile = tile.astype(jnp.bfloat16)
        dense[0, block] = tile[:half]
        dense[1, block] = tile[half:]
        return carry

    linked[pl.ds(pl.multiple_of(me * rows, rows), rows), :] = feat_ref[...]
    back[core, me] = jnp.zeros((half, rows), jnp.bfloat16)
    afeat[core] = afeat_ref[...]

    pl.semaphore_wait(barrier, count)

    def to_core(source, target, slot):
        return to_other_core(source, target, core_send, core_recv, slot, other)

    def tile_copy(step):
        block = lax.rem(me + step, count)
        return pltpu.make_async_remote_copy(
            src_ref=dense.at[core, block],
            dst_ref=back.at[core, me],
            send_sem=tile_send.at[step],
            recv_sem=tile_recv.at[step],
            device_id={"blk": block},
            device_id_type=MESH,
        )

    afeat_copy = to_core(afeat.at[core], afeat.at[core], 0)
    back_copy = to_core(back.at[core], back.at[core], 1)

    def direct(step):
        return pltpu.make_async_remote_copy(
            src_ref=feat_ref,
            dst_ref=linked.at[pl.ds(pl.multiple_of(me * rows, rows), rows)],
            send_sem=relay_send.at[step],
            recv_sem=relay_recv.at[step],
            device_id={"blk": lax.rem(me + step, count)},
            device_id_type=MESH,
        )

    def run(body):
        def one(step, carry):
            body(step)
            return carry

        lax.fori_loop(1, count, one, 0)

    run(lambda step: direct(step).start())
    lax.fori_loop(0, count, fill, 0)
    run(lambda step: tile_copy(step).start())
    afeat_copy.start()
    for weight in weights:
        weight.start()
    run(lambda step: tile_copy(step).wait())
    back_copy.start()
    back_copy.wait()

    def mix(block, carry):
        own = jnp.concatenate([dense[0, block], dense[1, block]], axis=0)
        came = jnp.concatenate([back[0, block], back[1, block]], axis=0)
        whole = own.astype(jnp.float32) + came.astype(jnp.float32).T
        mixed[:, pl.ds(pl.multiple_of(block * rows, rows), rows)] = whole.astype(jnp.bfloat16)
        return carry

    lax.fori_loop(0, count, mix, 0)
    run(lambda step: direct(step).wait())

    span = min(count * rows, 2048)

    def product(step, total):
        start = pl.multiple_of(step * span, span)
        return total + jnp.dot(
            mixed[:, pl.ds(start, span)],
            linked[pl.ds(start, span), :],
            preferred_element_type=jnp.float32,
        )

    total = feat_ref[...].astype(jnp.float32)
    total = lax.fori_loop(0, count * rows // span, product, total)
    pre[core] = total.astype(jnp.bfloat16)
    pre_copy = to_core(pre.at[core], pre.at[core], 2)
    pre_copy.start()

    member_matrix, member_back, inverse = membership(assign_ref, afeat_ref.shape[0], rows)
    weights[0].wait()
    own_units, own_square = scaled_units(pre, core, width, p_gain_ref, w_p_in)
    pre_copy.wait()
    far_units, far_square = scaled_units(pre, other, width, p_gain_ref, w_p_in)
    scale = lax.rsqrt((own_square + far_square) / (2 * width) + epsilon)
    hidden = silu((own_units + far_units) * scale)
    afeat_copy.wait()
    after_hidden(
        core,
        hidden,
        member_matrix,
        member_back,
        inverse,
        weights,
        to_core,
        (3, 4, 5),
        afeat,
        pre,
        w_p_out,
        w_a_in,
        w_a_out,
        a_gain_ref,
        partial_send,
        partial_recv,
        apart_send,
        apart_recv,
        mid,
        author_pre,
        result_ref,
    )


def local(
    features,
    partners,
    tiles,
    paper_w_in,
    paper_w_out,
    paper_gain,
    author_feats,
    assign,
    author_w_in,
    author_w_out,
    author_gain,
):
    count = lax.axis_size("blk")
    rows, width = features.shape
    bf16 = jnp.bfloat16
    f32 = jnp.float32
    vmem = pl.BlockSpec(memory_space=pltpu.VMEM)
    hbm = pl.BlockSpec(memory_space=pl.ANY)
    smem = pl.BlockSpec(memory_space=pltpu.SMEM)
    dma = pltpu.SemaphoreType.DMA
    pair = pltpu.VMEM((2, rows, width), bf16)
    single = pltpu.VMEM(author_feats.shape, bf16)
    held = [
        pltpu.VMEM(paper_w_in.shape, bf16),
        pltpu.VMEM(paper_w_out.shape, bf16),
        pltpu.VMEM(author_w_in.shape, bf16),
        pltpu.VMEM(author_w_out.shape, bf16),
    ]
    if count == PLANE * RING and width % LANES == 0:
        chunks = width // LANES
        body = grid_kernel
        near = hbm
        scratch = held + [
            pltpu.VMEM(tiles.shape[1:], bf16),
            pltpu.VMEM((PLANE, rows, RING * rows), bf16),
            pltpu.VMEM((RING, rows, PLANE * rows), bf16),
            pltpu.VMEM((PLANE, rows, RING * rows), bf16),
            pltpu.VMEM((RING, rows, PLANE * rows), bf16),
            pltpu.VMEM((PLANE * rows, RING * rows), bf16),
            pltpu.VMEM((chunks, RING * rows, LANES), bf16),
            pltpu.VMEM((chunks, PLANE * rows, LANES), f32),
            pltpu.VMEM((chunks, PLANE, rows, LANES), bf16),
            pltpu.VMEM((chunks, PLANE - 1, rows, LANES), bf16),
            pair,
            pair,
            pair,
            pair,
            single,
            single,
            pair,
            pair,
            dma((4,)),
            dma((chunks + 2,)),
            dma((chunks * 3,)),
            dma((chunks * RING,)),
            dma((PLANE + RING,)),
            dma((PLANE + RING,)),
            dma((chunks * (PLANE - 1),)),
            dma((chunks * (PLANE - 1),)),
            dma((2 * PLANE + 2 + chunks,)),
            dma((2 * PLANE + 2 + chunks,)),
        ]
    else:
        body = direct_kernel
        near = vmem
        tile_half = pltpu.VMEM((2, count, rows // 2, rows), bf16)
        scratch = held + [
            tile_half,
            tile_half,
            pltpu.VMEM((count * rows, width), bf16),
            pltpu.VMEM((rows, count * rows), bf16),
            pair,
            pair,
            pair,
            pair,
            single,
            single,
            pair,
            pair,
            dma((4,)),
            dma((count,)),
            dma((count,)),
            dma((count,)),
            dma((count,)),
            dma((6,)),
            dma((6,)),
        ]
    (result,) = pl.pallas_call(
        functools.partial(body, count),
        out_shape=(pltpu.VMEM((2,) + features.shape, bf16),),
        in_specs=[smem, near, near, hbm, hbm, vmem, near, vmem, hbm, hbm, vmem],
        out_specs=(vmem,),
        scratch_shapes=scratch,
        compiler_params=pltpu.CompilerParams(
            collective_id=0, has_side_effects=True, vmem_limit_bytes=56 * 1024 * 1024
        ),
    )(
        partners,
        tiles,
        features,
        paper_w_in,
        paper_w_out,
        paper_gain[None, :],
        author_feats,
        assign[None, :],
        author_w_in,
        author_w_out,
        author_gain[None, :],
    )
    return result[0], result[1]


def solution(mesh):
    placed = (
        P("blk", "auth"),
        P("blk", None),
        P("blk", None, None, None),
        P(None, "auth"),
        P("auth", None),
        P(),
        P("blk", "auth"),
        P("blk"),
        P(None, "auth"),
        P("auth", None),
        P(),
    )
    return jax.shard_map(
        local,
        mesh=mesh,
        in_specs=placed,
        out_specs=(P("blk", "auth"), P("blk", "auth")),
        check_vma=False,
    )
```
